512 devices in a mesh: blk: 32 (over z, y_hi), grp: 16 (over x, y_lo, core).
Axes of the slice: x: 4, y: 4 (y_hi: 2, y_lo: 2; y = y_hi * 2 + y_lo), z: 16, core: 2. Of those that a mesh axis runs over, the one named last changes fastest.
Arguments:
- embeddings: bfloat16 [65536, 1024], P(('blk', 'grp')), may hold values from -100 to 100
- labels: int32 [65536], P(('blk', 'grp')), may hold values from 0 to 66439, as said below
Outputs:
- anchor_loss: float32 [16384], P(('blk', 'grp'))
- mean_loss: float32 [], replicated
The draws below stay inside these ranges and needn't reach their ends.
Inputs may be any that keep to these rules, and one draw needn't show every extreme that they name: `labels`: A label of 1000 or more belongs to one sample only.
All inputs are finite; a program needn't handle non-finite values.
Results may differ from the reference program's by a relative error of at most 0.0003.
Values may be sent and summed in bfloat16 or wider, within the bound.
No kernel may reach another device: no remote copies, remote signals or barrier semaphores. Data moves between devices by JAX's collectives and lax.ppermute only.
A program may use at most 64 MiB of HBM per device.

```python
import math
import jax
import jax.numpy as jnp
from jax import lax

D = 1024
B_DEV = 128
A_DEV = 32
CLASSES = 1000
TOTAL = 65536


def class_labels(key):
    base_key = jax.random.fold_in(key, 11)
    sub_keys = jax.random.split(base_key, 6)
    smallest = jnp.full((TOTAL,), CLASSES - 1, jnp.int32)
    for draw_step in range(4):
        smallest = jnp.minimum(smallest, jax.random.randint(sub_keys[draw_step], (TOTAL,), 0, CLASSES, dtype=jnp.int32))
    class_order = jax.random.permutation(sub_keys[4], jnp.arange(CLASSES, dtype=jnp.int32))
    common_label = class_order[smallest]
    sample_ids = jnp.arange(TOTAL, dtype=jnp.int32)
    common_label = jnp.where(sample_ids == 0, 0, common_label)
    is_anchor = sample_ids % B_DEV < A_DEV
    lone_label = is_anchor & (jax.random.randint(sub_keys[5], (TOTAL,), 0, 16, dtype=jnp.int32) == 0)
    lone_label = lone_label & (sample_ids != 0)
    lone_label = lone_label | (sample_ids == TOTAL - B_DEV + A_DEV - 1)
    return jnp.where(lone_label, CLASSES + sample_ids, common_label).astype(jnp.int32)


def draw_labels(key, part):
    return class_labels(key)


def draw_embeddings(key, part):
    sample_labels = class_labels(key)
    centre_key, noise_key = jax.random.split(jax.random.fold_in(key, 23), 2)
    centroids = jax.random.normal(centre_key, (CLASSES, D), jnp.float32)
    has_class = (sample_labels < CLASSES).astype(jnp.float32)
    class_rows = centroids[jnp.minimum(sample_labels, CLASSES - 1)] * has_class[:, None]
    noise_part = jax.random.normal(noise_key, (TOTAL, D), jnp.float32)
    drawn = 0.8 * class_rows + noise_part
    return jnp.clip(drawn, -100.0, 100.0).astype(jnp.bfloat16)


def setup_inputs(seed: int = 0) -> dict:
    arg_keys = jax.random.split(jax.random.key(seed), 3)
    return {
        "embeddings": draw_embeddings(jax.random.fold_in(arg_keys[2], 71), 0),
        "labels": draw_labels(jax.random.fold_in(arg_keys[2], 71), 0),
    }


def reference(embeddings, labels):
    values = embeddings.astype(jnp.float32)
    unit = (values * lax.rsqrt(lax.optimization_barrier(jnp.sum(values * values, axis=1, keepdims=True)) + 1e-06)).astype(jnp.bfloat16)
    total = unit.shape[0]
    shards = total // B_DEV
    anchor_unit = unit.reshape(shards, B_DEV, unit.shape[1])[:, :A_DEV].reshape(shards * A_DEV, unit.shape[1])
    anchor_lab = labels.reshape(shards, B_DEV)[:, :A_DEV].reshape(shards * A_DEV)
    shard_ids = jnp.arange(shards, dtype=jnp.int32)[:, None] * B_DEV
    anchor_pos = (shard_ids + jnp.arange(A_DEV, dtype=jnp.int32)[None, :]).reshape(shards * A_DEV)
    anchors_all = shards * A_DEV
    width = math.gcd(anchors_all, 512)
    blocks = anchors_all // width
    key_ids = jnp.arange(total, dtype=jnp.int32)

    def one_block(index):
        start = (index * width).astype(jnp.int32)
        anchors = lax.dynamic_slice_in_dim(anchor_unit, start, width, 0)
        anchor_labels = lax.dynamic_slice_in_dim(anchor_lab, start, width, 0)
        anchor_ids = lax.dynamic_slice_in_dim(anchor_pos, start, width, 0)
        score = lax.dot_general(anchors, unit, (((1,), (1,)), ((), ())), preferred_element_type=jnp.float32) * 10.0
        self_mask = anchor_ids[:, None] == key_ids[None, :]
        denom = lax.optimization_barrier(jnp.sum(jnp.where(self_mask, 0.0, jnp.exp(score - 10.0)), axis=1))
        positive = (anchor_labels[:, None] == labels[None, :]) & jnp.logical_not(self_mask)
        pos_sum = lax.optimization_barrier(jnp.sum(jnp.where(positive, score, 0.0), axis=1))
        count = lax.optimization_barrier(jnp.sum(positive.astype(jnp.float32), axis=1))
        return (denom, pos_sum, count)
    denom, pos_sum, count = lax.map(one_block, jnp.arange(blocks, dtype=jnp.int32))
    denom = denom.reshape(anchors_all)
    pos_sum = pos_sum.reshape(anchors_all)
    count = count.reshape(anchors_all)
    valid = count > 0.0
    anchor_loss = jnp.where(valid, jnp.log(denom) + 10.0 - pos_sum / jnp.maximum(count, 1.0), 0.0)
    mean_loss = jnp.sum(anchor_loss) / jnp.maximum(jnp.sum(valid.astype(jnp.float32)), 1.0)
    return (anchor_loss, mean_loss)
```

```python
import jax
import jax.numpy as jnp
from jax import lax
from jax.sharding import Mesh
from jax.sharding import PartitionSpec as P

A_DEV = 32
HALF = 64
LAB = 8
ALL = ("zh", "zl", "Y", "x", "y", "c")
Z = ("zh", "zl")
YY = ("Y", "y")
PLANE = ("Y", "x", "y", "c")


def to_all(block, axis):
    devices = lax.axis_size(axis)
    return lax.all_to_all(
        jnp.broadcast_to(block[None], (devices, *block.shape)), axis, 0, 0, tiled=True
    )


def shifted(block, axis, step):
    devices = lax.axis_size(axis)
    return lax.ppermute(block, axis, [(i, (i + step) % devices) for i in range(devices)])


def label_rows(labels):
    high = (labels + 256) >> 9
    low = labels - high * 512
    digits = jnp.concatenate([high, low]).astype(jnp.bfloat16)
    row = jnp.pad(digits, (0, 1024 - digits.shape[0]))
    return jnp.pad(row[None], ((0, LAB - 1), (0, 0)))


def labels_of(rows, count):
    values = rows.astype(jnp.float32)
    return values[..., :count] * 512.0 + values[..., count : 2 * count]


def local(embeddings, labels):
    values = embeddings.astype(jnp.float32)
    unit = (values * lax.rsqrt(jnp.sum(values * values, axis=1, keepdims=True) + 1e-06)).astype(
        jnp.bfloat16
    )
    zh, zl = lax.axis_index("zh"), lax.axis_index("zl")
    plane_at = lax.axis_index(PLANE)
    cores = lax.axis_index("c")

    anchor_block = jnp.concatenate([unit[:A_DEV], label_rows(labels[:A_DEV])])
    first = jnp.concatenate([unit[:HALF], label_rows(labels)])
    second = unit[HALF:]

    far = to_all(anchor_block, "zh")
    keys_x = to_all(first, "x")
    keys_y = to_all(second, YY)
    behind = shifted(far, Z, 1)
    ahead = shifted(far, Z, -1)
    behind_2 = shifted(far[:2], Z, 2)
    ahead_2 = shifted(far[2:], Z, -2)
    keys_xy = to_all(keys_x, YY).reshape(4, 4, HALF + LAB, 1024)
    keys_yx = to_all(keys_y, "x").reshape(4, 4, HALF, 1024)
    other_xy = shifted(keys_xy, "c", 1)
    other_yx = shifted(keys_yx, "c", 1)

    anchors_all = jnp.stack([far, ahead, jnp.concatenate([behind_2, ahead_2]), behind])
    anchors = anchors_all[:, :, :A_DEV].reshape(16 * A_DEV, 1024)
    anchor_labels = labels_of(anchors_all[:, :, A_DEV], A_DEV).reshape(16 * A_DEV)
    own = jnp.arange(16 * A_DEV, dtype=jnp.int32)
    is_own_block = (own // A_DEV) == zh

    def sums(keys_first, keys_second, own_core):
        key_labels = labels_of(keys_first[:, :, HALF], 2 * HALF)
        firsts = keys_first[:, :, :HALF]
        keys = jnp.concatenate(
            [firsts.reshape(-1, 1024), keys_second.reshape(-1, 1024)]
        )
        key_labels = jnp.concatenate(
            [key_labels[..., :HALF].reshape(-1), jnp.swapaxes(key_labels[..., HALF:], 0, 1).reshape(-1)]
        )
        at = jnp.arange(keys.shape[0], dtype=jnp.int32)
        yy_x = lax.axis_index(YY) * 4 + lax.axis_index("x")
        own_row = jnp.where(own_core & (at < 1024) & (at // HALF == yy_x), at % HALF, -1)
        own_anchor = jnp.where(is_own_block, own % A_DEV, -2)
        score = (
            lax.dot_general(
                keys, anchors, (((1,), (1,)), ((), ())), preferred_element_type=jnp.float32
            )
            * 10.0
        )
        self_mask = own_row[:, None] == own_anchor[None, :]
        expo = jnp.where(self_mask, 0.0, jnp.exp(score - 10.0))
        positive = (key_labels[:, None] == anchor_labels[None, :]) & jnp.logical_not(self_mask)
        return jnp.stack(
            [
                jnp.sum(expo, axis=0),
                jnp.sum(jnp.where(positive, score, 0.0), axis=0),
                jnp.sum(positive.astype(jnp.float32), axis=0),
            ]
        )

    partial = sums(keys_xy, keys_yx, True) + sums(other_xy, other_yx, False)
    partial = partial.reshape(3, 4, 4, A_DEV)
    partial = jnp.roll(partial, zl, axis=1)
    arrived = to_all(partial.reshape(12, 128), Z).sum(axis=0).reshape(3, 16, A_DEV)
    denom, pos_sum, count = arrived
    valid = count > 0.0
    loss = jnp.where(valid, jnp.log(denom) + 10.0 - pos_sum / jnp.maximum(count, 1.0), 0.0)
    anchor_loss = lax.dynamic_index_in_dim(loss, zl * 4 + zh, 0, keepdims=False)
    both = jnp.stack([jnp.sum(loss), jnp.sum(valid.astype(jnp.float32))])
    everyone = to_all(jnp.broadcast_to(both[:, None], (2, 128)), PLANE).sum(axis=0)[:, 0]
    mean_loss = everyone[0] / jnp.maximum(everyone[1], 1.0)
    return (anchor_loss, mean_loss)


def solution(mesh):
    torus = Mesh(mesh.devices.reshape(4, 4, 2, 4, 2, 2), ALL)
    placed = (P(ALL, None), P(ALL))
    return jax.shard_map(
        local, mesh=torus, in_specs=placed, out_specs=(P(ALL), P()), check_vma=False
    )
```

```python
import jax
import jax.numpy as jnp
from jax import lax
from jax.experimental import pallas as pl
from jax.experimental.pallas import tpu as pltpu
from jax.sharding import Mesh
from jax.sharding import PartitionSpec as P

D = 1024
A_DEV = 32
KEYS = 128
LAB = 8
X = 4
Y = 4
Z = 16
ROWS = KEYS + LAB
HALF = KEYS // 2 + LAB
SIDE = A_DEV + LAB
F32 = jnp.float32
BF16 = jnp.bfloat16


def device_at(z, x, y, c):
    return ((((z % Z) * 2 + (y % Y) // 2) * X + x % X) * 2 + y % 2) * 2 + c


SPOTS = [(z, x, y, c) for z in range(Z) for x in range(X) for y in range(Y) for c in range(2)]
COLUMNS = [
    [device_at(z, x, y, c) for z in range(Z)] for x in range(X) for y in range(Y) for c in range(2)
]
PLANES = [
    [device_at(z, x, y, c) for x in range(X) for y in range(Y) for c in range(2)] for z in range(Z)
]


def moved(block, target):
    return lax.ppermute(block, "d", [(device_at(*spot), device_at(*target(*spot))) for spot in SPOTS])


def along_z(block, step):
    return moved(block, lambda z, x, y, c: (z + step, x, y, c))


def along_first(block, step):
    return moved(
        block, lambda z, x, y, c: (z, x + step, y, c) if c == 0 else (z, x, y + step, c)
    )


def along_second(block, step):
    return moved(
        block, lambda z, x, y, c: (z, x, y + step, c) if c == 0 else (z, x + step, y, c)
    )


def other_core(block):
    return moved(block, lambda z, x, y, c: (z, x, y, 1 - c))


def swapped_to_all(blocks, groups):
    return lax.all_to_all(blocks, "d", 0, 0, tiled=True, axis_index_groups=groups)


def vmem():
    return pl.BlockSpec(memory_space=pltpu.VMEM)


def smem():
    return pl.BlockSpec(memory_space=pltpu.SMEM)


def call(body, n_in, outs, scratch=(), limit=8):
    return pl.pallas_call(
        body,
        in_specs=[smem()] + [vmem()] * n_in,
        out_specs=jax.tree.map(lambda _: vmem(), outs),
        out_shape=outs,
        scratch_shapes=list(scratch),
        compiler_params=pltpu.CompilerParams(vmem_limit_bytes=limit * 1024 * 1024),
    )


def prepare_body(at, emb, labels, keys, anchors):
    values = emb[...].astype(F32)
    scale = lax.rsqrt(jnp.sum(values * values, axis=1, keepdims=True) + 1e-06)
    unit = (values * scale).astype(BF16)
    keys[:KEYS, :] = unit
    anchors[:A_DEV, :] = unit[:A_DEV]
    label = jnp.broadcast_to(labels[...], (8, KEYS))
    high = (label + 256) >> 9
    low = label - high * 512
    top = lax.broadcasted_iota(jnp.int32, (8, KEYS), 0) == 0
    lane = lax.broadcasted_iota(jnp.int32, (8, KEYS), 1)
    blank = jnp.zeros((8, D - 2 * KEYS), BF16)
    keys[KEYS:, 2 * KEYS :] = blank
    anchors[A_DEV:, 2 * KEYS :] = blank
    for k, digit in enumerate((high, low)):
        digit = jnp.where(top, digit.astype(F32), 0.0)
        keys[KEYS:, k * KEYS : (k + 1) * KEYS] = digit.astype(BF16)
        mine = pltpu.roll(jnp.where(lane < A_DEV, digit, 0.0), at[0] * A_DEV, 1)
        anchors[A_DEV:, k * KEYS : (k + 1) * KEYS] = mine.astype(BF16)


def far_body(at, own, before, after, across, far, low, high):
    zh = at[0]
    tail = None
    for step, ref in ((0, own), (3, before), (1, after), (2, across)):
        slot = (zh + step) % 4
        block = ref[:A_DEV, :]
        far[pl.ds(pl.multiple_of(slot * A_DEV, A_DEV), A_DEV), :] = block
        label = ref[A_DEV:, :].astype(F32)
        tail = label if tail is None else tail + label
    tail = tail.astype(BF16)
    far[KEYS:, :] = tail
    low[: KEYS // 2, :] = far[: KEYS // 2, :]
    high[: KEYS // 2, :] = far[KEYS // 2 : KEYS, :]
    low[KEYS // 2 :, :] = tail
    high[KEYS // 2 :, :] = tail


def line_body(at, a, b, c, d, line):
    for k, ref in enumerate((a, b, c, d)):
        line[k] = ref[...]


def label_of(rows):
    rows = rows.astype(F32)
    return rows[:1, :KEYS] * 512.0 + rows[:1, KEYS : 2 * KEYS]


def scores_body(at, *refs):
    pieces = refs[:8]
    far, ahead, low, high, behind, out, anchors = refs[8:]
    zh, zl = at[0], at[1]
    n = KEYS
    anchors[0:n, :] = far[:n, :]
    anchors[n : 2 * n, :] = ahead[:n, :]
    anchors[2 * n : 2 * n + n // 2, :] = low[: n // 2, :]
    anchors[2 * n + n // 2 : 3 * n, :] = high[: n // 2, :]
    anchors[3 * n : 4 * n, :] = behind[:n, :]
    labels = [
        label_of(far[n:, :]),
        label_of(ahead[n:, :]),
        label_of(low[n // 2 :, :]),
        label_of(behind[n:, :]),
    ]
    shift = zh * A_DEV
    totals = [[jnp.zeros((8, n), F32) for _ in range(3)] for _ in range(4)]
    for p, piece in enumerate(pieces):
        for half in range(2):
            keys = piece[2 * half : 2 * half + 2, :n, :].reshape(2 * n, D)
            raw = lax.dot_general(
                keys, anchors[...], (((1,), (1,)), ((), ())), preferred_element_type=F32
            )
            for b in range(2):
                key_label = label_of(piece[2 * half + b, n:, :])
                key_label = jnp.broadcast_to(key_label, (n, n)).T
                for d in range(4):
                    score = raw[b * n : (b + 1) * n, d * n : (d + 1) * n] * 10.0
                    expo = jnp.exp(score - 10.0)
                    positive = key_label == labels[d]
                    if p == 0 and half == 0 and b == 0 and d == 0:
                        row = lax.broadcasted_iota(jnp.int32, (n, n), 0)
                        lane = lax.broadcasted_iota(jnp.int32, (n, n), 1)
                        itself = (row < A_DEV) & (row + shift == lane)
                        expo = jnp.where(itself, 0.0, expo)
                        positive = positive & jnp.logical_not(itself)
                    parts = (
                        expo,
                        jnp.where(positive, score, 0.0),
                        jnp.where(positive, 1.0, 0.0),
                    )
                    for k, part in enumerate(parts):
                        totals[d][k] += part.reshape(n // 8, 8, n).sum(axis=0)
    for d in range(4):
        slot = (zl + d) % 4
        for k in range(3):
            row = jnp.sum(totals[d][k], axis=0, keepdims=True)
            for z in range(Z):
                out[z, k, pl.ds(slot, 1), :] = row


def loss_body(at, arrived, own, both):
    zh, zl = at[0], at[1]
    total = arrived[0]
    for z in range(1, Z):
        total = total + arrived[z]
    denom, pos_sum, count = total[0], total[1], total[2]
    valid = count > 0.0
    loss = jnp.where(valid, jnp.log(denom) + 10.0 - pos_sum / jnp.maximum(count, 1.0), 0.0)
    classes = lax.broadcasted_iota(jnp.int32, loss.shape, 0)
    mine = jnp.sum(jnp.where(classes == zl, loss, 0.0), axis=0, keepdims=True)
    mine = jnp.broadcast_to(mine, (8, KEYS))
    own[...] = pltpu.roll(mine, (4 - zh) % 4 * A_DEV, 1)
    lane = lax.broadcasted_iota(jnp.int32, (1, KEYS), 1)
    loss_sum = jnp.sum(jnp.sum(loss, axis=0, keepdims=True), axis=1, keepdims=True)
    valid_sum = jnp.sum(
        jnp.sum(jnp.where(valid, 1.0, 0.0), axis=0, keepdims=True), axis=1, keepdims=True
    )
    row = jnp.where(lane == 0, loss_sum, jnp.where(lane == 1, valid_sum, 0.0))
    for k in range(2 * X * Y):
        both[k] = row


def loss_of(embeddings, labels):
    device = lax.axis_index("d")
    z = device // 32
    at = jnp.stack([z // 4, z % 4]).astype(jnp.int32)

    own_keys, own_anchors = call(
        prepare_body,
        2,
        (jax.ShapeDtypeStruct((ROWS, D), BF16), jax.ShapeDtypeStruct((SIDE, D), BF16)),
    )(at, embeddings, labels.reshape(1, KEYS))

    two = along_first(own_keys, 2)
    plus = along_first(own_keys, 1)
    minus = along_first(own_keys, -1)
    across = along_z(own_anchors, 8)
    before = along_z(own_anchors, 4)
    after = along_z(own_anchors, -4)

    (line,) = call(line_body, 4, (jax.ShapeDtypeStruct((4, ROWS, D), BF16),))(
        at, own_keys, plus, minus, two
    )
    line_two = along_second(line, 2)
    line_plus = along_second(line, 1)
    line_minus = along_second(line, -1)

    far, low, high = call(
        far_body,
        4,
        (
            jax.ShapeDtypeStruct((ROWS, D), BF16),
            jax.ShapeDtypeStruct((HALF, D), BF16),
            jax.ShapeDtypeStruct((HALF, D), BF16),
        ),
    )(at, own_anchors, before, after, across)
    low_in = along_z(low, 2)
    high_in = along_z(high, -2)
    behind = along_z(far, 1)
    ahead = along_z(far, -1)

    mine = [line, line_plus, line_minus, line_two]
    theirs = []
    for block in mine:
        theirs.append(other_core(block))

    (sums,) = call(
        scores_body,
        13,
        (jax.ShapeDtypeStruct((Z, 3, 4, KEYS), F32),),
        [pltpu.VMEM((4 * KEYS, D), BF16)],
        24,
    )(at, *mine, *theirs, far, ahead, low_in, high_in, behind)
    arrived = swapped_to_all(sums, COLUMNS)
    own_loss, both = call(
        loss_body,
        1,
        (
            jax.ShapeDtypeStruct((8, KEYS), F32),
            jax.ShapeDtypeStruct((2 * X * Y, 1, KEYS), F32),
        ),
    )(at, arrived)
    everyone = swapped_to_all(both, PLANES).sum(axis=0)[0]
    mean_loss = everyone[0] / jnp.maximum(everyone[1], 1.0)
    return (own_loss[0, :A_DEV], mean_loss)


def solution(mesh):
    flat = Mesh(mesh.devices.reshape(512), ("d",))
    placed = (P("d", None), P("d"))
    return jax.shard_map(
        loss_of, mesh=flat, in_specs=placed, out_specs=(P("d"), P()), check_vma=False
    )
```

```python
import jax
import jax.numpy as jnp
from jax import lax
from jax.experimental import pallas as pl
from jax.experimental.pallas import tpu as pltpu
from jax.sharding import Mesh
from jax.sharding import PartitionSpec as P

D = 1024
A_DEV = 32
KEYS = 128
LAB = 8
X = 4
Y = 4
Z = 16
ROWS = KEYS + LAB
SIDE = A_DEV + LAB
F32 = jnp.float32
BF16 = jnp.bfloat16


def device_at(z, x, y, c):
    return ((((z % Z) * 2 + (y % Y) // 2) * X + x % X) * 2 + y % 2) * 2 + c


SPOTS = [(z, x, y, c) for z in range(Z) for x in range(X) for y in range(Y) for c in range(2)]
LINES = [[device_at(z, k, y, 0) for k in range(X)] for z in range(Z) for y in range(Y)] + [
    [device_at(z, x, k, 1) for k in range(Y)] for z in range(Z) for x in range(X)
]
CROSS_LINES = [[device_at(z, x, k, 0) for k in range(Y)] for z in range(Z) for x in range(X)] + [
    [device_at(z, k, y, 1) for k in range(X)] for z in range(Z) for y in range(Y)
]
COLUMNS = [
    [device_at(z, x, y, c) for z in range(Z)] for x in range(X) for y in range(Y) for c in range(2)
]
PLANES = [
    [device_at(z, x, y, c) for x in range(X) for y in range(Y) for c in range(2)] for z in range(Z)
]


def moved(block, target):
    return lax.ppermute(block, "d", [(device_at(*spot), device_at(*target(*spot))) for spot in SPOTS])


def along_z(block, step):
    return moved(block, lambda z, x, y, c: (z + step, x, y, c))


def two_along_z(block):
    return moved(block, lambda z, x, y, c: (z + 2 - 4 * c, x, y, c))


def other_core(block):
    return moved(block, lambda z, x, y, c: (z, x, y, 1 - c))


def swapped_to_all(blocks, groups):
    return lax.all_to_all(blocks, "d", 0, 0, tiled=True, axis_index_groups=groups)


def vmem():
    return pl.BlockSpec(memory_space=pltpu.VMEM)


def smem():
    return pl.BlockSpec(memory_space=pltpu.SMEM)


def call(body, n_in, outs, scratch=(), limit=8):
    return pl.pallas_call(
        body,
        in_specs=[smem()] + [vmem()] * n_in,
        out_specs=jax.tree.map(lambda _: vmem(), outs),
        out_shape=outs,
        scratch_shapes=list(scratch),
        compiler_params=pltpu.CompilerParams(vmem_limit_bytes=limit * 1024 * 1024),
    )


def prepare_body(at, emb, labels, keys, anchors):
    values = emb[...].astype(F32)
    scale = lax.rsqrt(jnp.sum(values * values, axis=1, keepdims=True) + 1e-06)
    unit = (values * scale).astype(BF16)
    for k in range(4):
        keys[k, :KEYS, :] = unit
    anchors[:A_DEV, :] = unit[:A_DEV]
    label = jnp.broadcast_to(labels[...], (8, KEYS))
    high = (label + 256) >> 9
    low = label - high * 512
    top = lax.broadcasted_iota(jnp.int32, (8, KEYS), 0) == 0
    lane = lax.broadcasted_iota(jnp.int32, (8, KEYS), 1)
    blank = jnp.zeros((8, D - 2 * KEYS), BF16)
    for k in range(4):
        keys[k, KEYS:, 2 * KEYS :] = blank
    anchors[A_DEV:, 2 * KEYS :] = blank
    for k, digit in enumerate((high, low)):
        digit = jnp.where(top, digit.astype(F32), 0.0)
        for copy in range(4):
            keys[copy, KEYS:, k * KEYS : (k + 1) * KEYS] = digit.astype(BF16)
        mine = pltpu.roll(jnp.where(lane < A_DEV, digit, 0.0), at[0] * A_DEV, 1)
        anchors[A_DEV:, k * KEYS : (k + 1) * KEYS] = mine.astype(BF16)


def far_body(at, own, before, after, across, far):
    zh = at[0]
    tail = None
    for step, ref in ((0, own), (3, before), (1, after), (2, across)):
        slot = (zh + step) % 4
        far[pl.ds(pl.multiple_of(slot * A_DEV, A_DEV), A_DEV), :] = ref[:A_DEV, :]
        label = ref[A_DEV:, :].astype(F32)
        tail = label if tail is None else tail + label
    far[KEYS:, :] = tail.astype(BF16)


def line_body(at, line, copies):
    for k in range(4):
        block = line[k]
        for copy in range(4):
            copies[copy, k] = block


def label_of(rows):
    rows = rows.astype(F32)
    return rows[:1, :KEYS] * 512.0 + rows[:1, KEYS : 2 * KEYS]


def scores_of(at, pieces, anchors_in, anchors, mine):
    n = KEYS
    labels = []
    for d, ref in enumerate(anchors_in):
        anchors[d * n : (d + 1) * n, :] = ref[:n, :]
        labels.append(label_of(ref[n:, :]))
    totals = [[jnp.zeros((8, n), F32) for _ in range(3)] for _ in range(4)]
    if mine:
        row = lax.broadcasted_iota(jnp.int32, (n, n), 0)
        lane = lax.broadcasted_iota(jnp.int32, (n, n), 1)
        diagonal = (row < A_DEV) & (row + at[0] * A_DEV == lane)
    for p in range(4):
        for half in range(2):
            keys = pieces[p, 2 * half : 2 * half + 2, :n, :].reshape(2 * n, D)
            raw = lax.dot_general(
                keys, anchors[...], (((1,), (1,)), ((), ())), preferred_element_type=F32
            )
            for b in range(2):
                key_label = label_of(pieces[p, 2 * half + b, n:, :])
                key_label = jnp.broadcast_to(key_label, (n, n)).T
                for d in range(4):
                    score = raw[b * n : (b + 1) * n, d * n : (d + 1) * n] * 10.0
                    expo = jnp.exp(score - 10.0)
                    positive = key_label == labels[d]
                    if mine and d == 0:
                        itself = diagonal & (at[2] == 4 * p + 2 * half + b)
                        expo = jnp.where(itself, 0.0, expo)
                        positive = positive & jnp.logical_not(itself)
                    parts = (
                        expo,
                        jnp.where(positive, score, 0.0),
                        jnp.where(positive, 1.0, 0.0),
                    )
                    for k, part in enumerate(parts):
                        totals[d][k] += part.reshape(n // 8, 8, n).sum(axis=0)
    return totals


def mine_body(at, pieces, far, ahead, across, behind, out, anchors):
    totals = scores_of(at, pieces, (far, ahead, across, behind), anchors, True)
    for d in range(4):
        for k in range(3):
            out[d, k] = totals[d][k]


def theirs_body(at, pieces, far, ahead, across, behind, before, out, anchors):
    totals = scores_of(at, pieces, (far, ahead, across, behind), anchors, False)
    for d in range(4):
        slot = (at[1] + d) % 4
        for k in range(3):
            row = jnp.sum(totals[d][k] + before[d, k], axis=0, keepdims=True)
            for z in range(Z):
                out[z, k, pl.ds(slot, 1), :] = row


def loss_body(at, arrived, own, both):
    zh, zl = at[0], at[1]
    total = arrived[0]
    for z in range(1, Z):
        total = total + arrived[z]
    denom, pos_sum, count = total[0], total[1], total[2]
    valid = count > 0.0
    loss = jnp.where(valid, jnp.log(denom) + 10.0 - pos_sum / jnp.maximum(count, 1.0), 0.0)
    classes = lax.broadcasted_iota(jnp.int32, loss.shape, 0)
    mine = jnp.sum(jnp.where(classes == zl, loss, 0.0), axis=0, keepdims=True)
    mine = jnp.broadcast_to(mine, (8, KEYS))
    own[...] = pltpu.roll(mine, (4 - zh) % 4 * A_DEV, 1)
    lane = lax.broadcasted_iota(jnp.int32, (1, KEYS), 1)
    loss_sum = jnp.sum(jnp.sum(loss, axis=0, keepdims=True), axis=1, keepdims=True)
    valid_sum = jnp.sum(
        jnp.sum(jnp.where(valid, 1.0, 0.0), axis=0, keepdims=True), axis=1, keepdims=True
    )
    row = jnp.where(lane == 0, loss_sum, jnp.where(lane == 1, valid_sum, 0.0))
    for k in range(2 * X * Y):
        both[k] = row


def loss_of(embeddings, labels):
    device = lax.axis_index("d")
    z = device // 32
    x = device // 4 % 4
    y = device // 16 % 2 * 2 + device // 2 % 2
    own_at = jnp.where(device % 2 == 0, y * 4 + x, x * 4 + y)
    at = jnp.stack([z // 4, z % 4, own_at]).astype(jnp.int32)

    own_keys, own_anchors = call(
        prepare_body,
        2,
        (jax.ShapeDtypeStruct((4, ROWS, D), BF16), jax.ShapeDtypeStruct((SIDE, D), BF16)),
    )(at, embeddings, labels.reshape(1, KEYS))

    line = swapped_to_all(own_keys, LINES)
    across = along_z(own_anchors, 8)
    before = along_z(own_anchors, 4)
    after = along_z(own_anchors, -4)

    (copies,) = call(line_body, 1, (jax.ShapeDtypeStruct((4, 4, ROWS, D), BF16),))(at, line)
    mine = swapped_to_all(copies, CROSS_LINES)

    (far,) = call(far_body, 4, (jax.ShapeDtypeStruct((ROWS, D), BF16),))(
        at, own_anchors, before, after, across
    )
    across_near = two_along_z(far)
    behind = along_z(far, 1)
    ahead = along_z(far, -1)
    theirs = other_core(mine)

    anchors = [far, ahead, across_near, behind]
    scratch = [pltpu.VMEM((4 * KEYS, D), BF16)]
    (first,) = call(
        mine_body, 5, (jax.ShapeDtypeStruct((4, 3, 8, KEYS), F32),), scratch, 16
    )(at, mine, *anchors)
    (sums,) = call(
        theirs_body, 6, (jax.ShapeDtypeStruct((Z, 3, 4, KEYS), F32),), scratch, 16
    )(at, theirs, *anchors, first)
    arrived = swapped_to_all(sums, COLUMNS)
    own_loss, both = call(
        loss_body,
        1,
        (
            jax.ShapeDtypeStruct((8, KEYS), F32),
            jax.ShapeDtypeStruct((2 * X * Y, 1, KEYS), F32),
        ),
    )(at, arrived)
    everyone = swapped_to_all(both, PLANES).sum(axis=0)[0]
    mean_loss = everyone[0] / jnp.maximum(everyone[1], 1.0)
    return (own_loss[0, :A_DEV], mean_loss)


def solution(mesh):
    flat = Mesh(mesh.devices.reshape(512), ("d",))
    placed = (P("d", None), P("d"))
    return jax.shard_map(
        loss_of, mesh=flat, in_specs=placed, out_specs=(P("d"), P()), check_vma=False
    )
```

```python
import jax
import jax.numpy as jnp
from jax import lax
from jax.experimental import pallas as pl
from jax.experimental.pallas import tpu as pltpu
from jax.sharding import Mesh
from jax.sharding import PartitionSpec as P

D = 1024
A_DEV = 32
KEYS = 128
LAB = 8
X = 4
Y = 4
Z = 16
ROWS = KEYS + LAB
SIDE = A_DEV + LAB
F32 = jnp.float32
BF16 = jnp.bfloat16


def device_at(z, x, y, c):
    return ((((z % Z) * 2 + (y % Y) // 2) * X + x % X) * 2 + y % 2) * 2 + c


SPOTS = [(z, x, y, c) for z in range(Z) for x in range(X) for y in range(Y) for c in range(2)]
LINES = [[device_at(z, k, y, 0) for k in range(X)] for z in range(Z) for y in range(Y)] + [
    [device_at(z, x, k, 1) for k in range(Y)] for z in range(Z) for x in range(X)
]
CROSS_LINES = [[device_at(z, x, k, 0) for k in range(Y)] for z in range(Z) for x in range(X)] + [
    [device_at(z, k, y, 1) for k in range(X)] for z in range(Z) for y in range(Y)
]
COLUMNS = [
    [device_at(z, x, y, c) for z in range(Z) for c in range(2)] for x in range(X) for y in range(Y)
]
PLANES = [
    [device_at(z, x, y, c) for x in range(X) for y in range(Y) for c in range(2)] for z in range(Z)
]


def moved(block, target):
    return lax.ppermute(block, "d", [(device_at(*spot), device_at(*target(*spot))) for spot in SPOTS])


def along_z(block, step):
    return moved(block, lambda z, x, y, c: (z + step, x, y, c))


def split_along_z(block, step):
    return moved(block, lambda z, x, y, c: (z + step - 2 * step * c, x, y, c))


def other_core(block):
    return moved(block, lambda z, x, y, c: (z, x, y, 1 - c))


def swapped_to_all(blocks, groups):
    return lax.all_to_all(blocks, "d", 0, 0, tiled=True, axis_index_groups=groups)


def vmem():
    return pl.BlockSpec(memory_space=pltpu.VMEM)


def smem():
    return pl.BlockSpec(memory_space=pltpu.SMEM)


def call(body, n_in, outs, scratch=(), limit=8):
    return pl.pallas_call(
        body,
        in_specs=[smem()] + [vmem()] * n_in,
        out_specs=jax.tree.map(lambda _: vmem(), outs),
        out_shape=outs,
        scratch_shapes=list(scratch),
        compiler_params=pltpu.CompilerParams(vmem_limit_bytes=limit * 1024 * 1024),
    )


def prepare_body(at, emb, labels, keys, anchors):
    values = emb[...].astype(F32)
    scale = lax.rsqrt(jnp.sum(values * values, axis=1, keepdims=True) + 1e-06)
    unit = (values * scale).astype(BF16)
    for k in range(4):
        keys[k, :KEYS, :] = unit
    anchors[:A_DEV, :] = unit[:A_DEV]
    label = jnp.broadcast_to(labels[...], (8, KEYS))
    high = (label + 256) >> 9
    low = label - high * 512
    top = lax.broadcasted_iota(jnp.int32, (8, KEYS), 0) == 0
    lane = lax.broadcasted_iota(jnp.int32, (8, KEYS), 1)
    blank = jnp.zeros((8, D - 2 * KEYS), BF16)
    for k in range(4):
        keys[k, KEYS:, 2 * KEYS :] = blank
    anchors[A_DEV:, 2 * KEYS :] = blank
    for k, digit in enumerate((high, low)):
        digit = jnp.where(top, digit.astype(F32), 0.0)
        for copy in range(4):
            keys[copy, KEYS:, k * KEYS : (k + 1) * KEYS] = digit.astype(BF16)
        mine = pltpu.roll(jnp.where(lane < A_DEV, digit, 0.0), at[0] * A_DEV, 1)
        anchors[A_DEV:, k * KEYS : (k + 1) * KEYS] = mine.astype(BF16)


def pair_body(at, own, across, pair):
    pair[:A_DEV, :] = own[:A_DEV, :]
    pair[A_DEV : 2 * A_DEV, :] = across[:A_DEV, :]
    tail = own[A_DEV:, :].astype(F32) + across[A_DEV:, :].astype(F32)
    pair[2 * A_DEV :, :] = tail.astype(BF16)


def far_body(at, pair, other, far):
    zh, c = at[0], at[3]
    for step, ref, k in ((0, pair, 0), (2, pair, 1), (3 + 2 * c, other, 0), (1 + 2 * c, other, 1)):
        slot = (zh + step) % 4
        block = ref[k * A_DEV : (k + 1) * A_DEV, :]
        far[pl.ds(pl.multiple_of(slot * A_DEV, A_DEV), A_DEV), :] = block
    tail = pair[2 * A_DEV :, :].astype(F32) + other[2 * A_DEV :, :].astype(F32)
    far[KEYS:, :] = tail.astype(BF16)


def copies_body(line, copies, done):
    moves = [pltpu.make_async_copy(line, copies.at[k], done.at[k]) for k in range(4)]
    for move in moves:
        move.start()
    for move in moves:
        move.wait()


def anchors_body(at, far, ahead, across, behind, anchors):
    row = lax.broadcasted_iota(jnp.int32, (LAB, D), 0)
    tail = jnp.zeros((LAB, D), F32)
    for d, ref in enumerate((far, ahead, across, behind)):
        anchors[d * KEYS : (d + 1) * KEYS, :] = ref[:KEYS, :]
        label = jnp.broadcast_to(ref[KEYS:, :].astype(F32)[:1], (LAB, D))
        tail = jnp.where(row == d, label, tail)
    anchors[4 * KEYS :, :] = tail.astype(BF16)


def label_of(rows):
    rows = rows.astype(F32)
    return rows[:, :KEYS] * 512.0 + rows[:, KEYS : 2 * KEYS]


def scores_of(at, block_of, sides, totals, has_own):
    n = KEYS
    if has_own:
        row = lax.broadcasted_iota(jnp.int32, (n, n), 0)
        lane = lax.broadcasted_iota(jnp.int32, (n, n), 1)
        diagonal = (row < A_DEV) & (row + at[0] * A_DEV == lane)
    for half in range(2):
        keys = block_of(2 * half, 2, slice(None, n)).reshape(2 * n, D)
        for s, anchors in enumerate(sides):
            labels = label_of(anchors[4 * n :, :])
            raw = lax.dot_general(
                keys, anchors[: 4 * n, :], (((1,), (1,)), ((), ())), preferred_element_type=F32
            )
            for b in range(2):
                rows = block_of(2 * half + b, 1, slice(n, None)).reshape(LAB, D)
                key_label = jnp.broadcast_to(label_of(rows)[:1], (n, n)).T
                for d in range(4):
                    score = raw[b * n : (b + 1) * n, d * n : (d + 1) * n] * 10.0
                    expo = jnp.exp(score - 10.0)
                    positive = key_label == labels[d : d + 1]
                    if has_own and s == 0 and d == 0:
                        itself = diagonal & (at[2] == 2 * half + b)
                        expo = jnp.where(itself, 0.0, expo)
                        positive = positive & jnp.logical_not(itself)
                    parts = (
                        expo,
                        jnp.where(positive, score, 0.0),
                        jnp.where(positive, 1.0, 0.0),
                    )
                    for k, part in enumerate(parts):
                        totals[s, d, k] += part.reshape(n // 8, 8, n).sum(axis=0)


def first_body(at, line, mine, theirs, totals):
    totals[...] = jnp.zeros(totals.shape, F32)
    scores_of(at, lambda k, m, rows: line[k : k + m, rows, :], (mine, theirs), totals, True)


def rest_body(at, plane, mine, theirs, before, out, totals):
    step = pl.program_id(0)

    @pl.when(step == 0)
    def _():
        totals[...] = before[...]

    scores_of(at, lambda k, m, rows: plane[0, k : k + m, rows, :], (mine, theirs), totals, False)

    @pl.when(step == 2)
    def _():
        for s in range(2):
            core = (at[3] + s) % 2
            for d in range(4):
                slot = (at[1] + d) % 4
                for k in range(3):
                    row = jnp.sum(totals[s, d, k], axis=0, keepdims=True)
                    for z in range(Z):
                        out[2 * z + core, k, pl.ds(slot, 1), :] = row


def loss_body(at, arrived, own, both):
    zh, zl = at[0], at[1]
    total = arrived[0]
    for z in range(1, 2 * Z):
        total = total + arrived[z]
    denom, pos_sum, count = total[0], total[1], total[2]
    valid = count > 0.0
    loss = jnp.where(valid, jnp.log(denom) + 10.0 - pos_sum / jnp.maximum(count, 1.0), 0.0)
    classes = lax.broadcasted_iota(jnp.int32, loss.shape, 0)
    mine = jnp.sum(jnp.where(classes == zl, loss, 0.0), axis=0, keepdims=True)
    mine = jnp.broadcast_to(mine, (8, KEYS))
    own[...] = pltpu.roll(mine, (4 - zh) % 4 * A_DEV, 1)
    lane = lax.broadcasted_iota(jnp.int32, (1, KEYS), 1)
    loss_sum = jnp.sum(jnp.sum(loss, axis=0, keepdims=True), axis=1, keepdims=True)
    valid_sum = jnp.sum(
        jnp.sum(jnp.where(valid, 1.0, 0.0), axis=0, keepdims=True), axis=1, keepdims=True
    )
    row = jnp.where(lane == 0, loss_sum, jnp.where(lane == 1, valid_sum, 0.0))
    for k in range(2 * X * Y):
        both[k] = row


def loss_of(embeddings, labels):
    device = lax.axis_index("d")
    c = device % 2
    z = device // 32
    x = device // 4 % 4
    y = device // 16 % 2 * 2 + device // 2 % 2
    in_line = jnp.where(c == 0, x, y)
    of_line = jnp.where(c == 0, y, x)
    at = jnp.stack([z // 4, z % 4, in_line, c, of_line]).astype(jnp.int32)

    own_keys, own_anchors = call(
        prepare_body,
        2,
        (jax.ShapeDtypeStruct((4, ROWS, D), BF16), jax.ShapeDtypeStruct((SIDE, D), BF16)),
    )(at, embeddings, labels.reshape(1, KEYS))

    line = swapped_to_all(own_keys, LINES)
    across = along_z(own_anchors, 8)

    copies = pl.pallas_call(
        copies_body,
        name="copies",
        in_specs=[vmem()],
        out_specs=pl.BlockSpec(memory_space=pltpu.HBM),
        out_shape=jax.ShapeDtypeStruct((4, 4, ROWS, D), BF16),
        scratch_shapes=[pltpu.SemaphoreType.DMA((4,))],
        compiler_params=pltpu.CompilerParams(vmem_limit_bytes=4 * 1024 * 1024),
    )(line)
    plane = swapped_to_all(copies, CROSS_LINES)

    two = jax.ShapeDtypeStruct((2 * A_DEV + LAB, D), BF16)
    (pair,) = call(pair_body, 2, (two,))(at, own_anchors, across)
    other_pair = split_along_z(pair, 4)
    (far,) = call(far_body, 2, (jax.ShapeDtypeStruct((ROWS, D), BF16),))(at, pair, other_pair)
    across_near = split_along_z(far, 2)
    behind = along_z(far, 1)
    ahead = along_z(far, -1)

    column = jax.ShapeDtypeStruct((4 * KEYS + LAB, D), BF16)
    (mine,) = call(anchors_body, 4, (column,))(at, far, ahead, across_near, behind)
    theirs = other_core(mine)

    sums_shape = (2, 4, 3, 8, KEYS)
    (first,) = call(first_body, 3, (jax.ShapeDtypeStruct(sums_shape, F32),), (), 16)(
        at, line, mine, theirs
    )
    whole = lambda dims: pl.BlockSpec(dims, lambda i, at: (0,) * len(dims))
    sums = pl.pallas_call(
        rest_body,
        name="rest",
        grid_spec=pltpu.PrefetchScalarGridSpec(
            num_scalar_prefetch=1,
            grid=(3,),
            in_specs=[
                pl.BlockSpec((1, 4, ROWS, D), lambda i, at: ((at[4] + 1 + i) % 4, 0, 0, 0)),
                whole(column.shape),
                whole(column.shape),
                whole(sums_shape),
            ],
            out_specs=whole((2 * Z, 3, 4, KEYS)),
            scratch_shapes=[pltpu.VMEM(sums_shape, F32)],
        ),
        out_shape=jax.ShapeDtypeStruct((2 * Z, 3, 4, KEYS), F32),
        compiler_params=pltpu.CompilerParams(vmem_limit_bytes=20 * 1024 * 1024),
    )(at, plane, mine, theirs, first)
    arrived = swapped_to_all(sums, COLUMNS)
    own_loss, both = call(
        loss_body,
        1,
        (
            jax.ShapeDtypeStruct((8, KEYS), F32),
            jax.ShapeDtypeStruct((2 * X * Y, 1, KEYS), F32),
        ),
    )(at, arrived)
    everyone = swapped_to_all(both, PLANES).sum(axis=0)[0]
    mean_loss = everyone[0] / jnp.maximum(everyone[1], 1.0)
    return (own_loss[0, :A_DEV], mean_loss)


def solution(mesh):
    flat = Mesh(mesh.devices.reshape(512), ("d",))
    placed = (P("d", None), P("d"))
    return jax.shard_map(
        loss_of, mesh=flat, in_specs=placed, out_specs=(P("d"), P()), check_vma=False
    )
```

```python
import jax
import jax.numpy as jnp
from jax import lax
from jax.experimental import pallas as pl
from jax.experimental.pallas import tpu as pltpu
from jax.sharding import Mesh
from jax.sharding import PartitionSpec as P

D = 1024
A_DEV = 32
KEYS = 128
LAB = 8
X = 4
Y = 4
Z = 16
ROWS = KEYS + LAB
SIDE = A_DEV + LAB
F32 = jnp.float32
BF16 = jnp.bfloat16


def device_at(z, x, y, c):
    return ((((z % Z) * 2 + (y % Y) // 2) * X + x % X) * 2 + y % 2) * 2 + c


SPOTS = [(z, x, y, c) for z in range(Z) for x in range(X) for y in range(Y) for c in range(2)]
LINES = [[device_at(z, k, y, 0) for k in range(X)] for z in range(Z) for y in range(Y)] + [
    [device_at(z, x, k, 1) for k in range(Y)] for z in range(Z) for x in range(X)
]
CROSS_LINES = [[device_at(z, x, k, 0) for k in range(Y)] for z in range(Z) for x in range(X)] + [
    [device_at(z, k, y, 1) for k in range(X)] for z in range(Z) for y in range(Y)
]
COLUMNS = [
    [device_at(z, x, y, c) for z in range(Z)] for x in range(X) for y in range(Y) for c in range(2)
]
PLANES = [
    [device_at(z, x, y, c) for x in range(X) for y in range(Y) for c in range(2)] for z in range(Z)
]


def moved(block, target):
    return lax.ppermute(block, "d", [(device_at(*spot), device_at(*target(*spot))) for spot in SPOTS])


def along_z(block, step):
    return moved(block, lambda z, x, y, c: (z + step, x, y, c))


def split_along_z(block, step):
    return moved(block, lambda z, x, y, c: (z + step - 2 * step * c, x, y, c))


def other_core(block):
    return moved(block, lambda z, x, y, c: (z, x, y, 1 - c))


def swapped_to_all(blocks, groups):
    return lax.all_to_all(blocks, "d", 0, 0, tiled=True, axis_index_groups=groups)


def vmem():
    return pl.BlockSpec(memory_space=pltpu.VMEM)


def smem():
    return pl.BlockSpec(memory_space=pltpu.SMEM)


def call(body, n_in, outs, scratch=(), limit=8):
    return pl.pallas_call(
        body,
        in_specs=[smem()] + [vmem()] * n_in,
        out_specs=jax.tree.map(lambda _: vmem(), outs),
        out_shape=outs,
        scratch_shapes=list(scratch),
        compiler_params=pltpu.CompilerParams(vmem_limit_bytes=limit * 1024 * 1024),
    )


def prepare_body(at, emb, labels, keys, anchors):
    values = emb[...].astype(F32)
    scale = lax.rsqrt(jnp.sum(values * values, axis=1, keepdims=True) + 1e-06)
    unit = (values * scale).astype(BF16)
    for k in range(4):
        keys[k, :KEYS, :] = unit
    anchors[:A_DEV, :] = unit[:A_DEV]
    label = jnp.broadcast_to(labels[...], (8, KEYS))
    high = (label + 256) >> 9
    low = label - high * 512
    top = lax.broadcasted_iota(jnp.int32, (8, KEYS), 0) == 0
    lane = lax.broadcasted_iota(jnp.int32, (8, KEYS), 1)
    blank = jnp.zeros((8, D - 2 * KEYS), BF16)
    for k in range(4):
        keys[k, KEYS:, 2 * KEYS :] = blank
    anchors[A_DEV:, 2 * KEYS :] = blank
    for k, digit in enumerate((high, low)):
        digit = jnp.where(top, digit.astype(F32), 0.0)
        for copy in range(4):
            keys[copy, KEYS:, k * KEYS : (k + 1) * KEYS] = digit.astype(BF16)
        mine = pltpu.roll(jnp.where(lane < A_DEV, digit, 0.0), at[0] * A_DEV, 1)
        anchors[A_DEV:, k * KEYS : (k + 1) * KEYS] = mine.astype(BF16)


def pair_body(at, own, across, pair):
    pair[:A_DEV, :] = own[:A_DEV, :]
    pair[A_DEV : 2 * A_DEV, :] = across[:A_DEV, :]
    tail = own[A_DEV:, :].astype(F32) + across[A_DEV:, :].astype(F32)
    pair[2 * A_DEV :, :] = tail.astype(BF16)


def far_body(at, pair, other, far):
    zh, c = at[0], at[3]
    for step, ref, k in ((0, pair, 0), (2, pair, 1), (3 + 2 * c, other, 0), (1 + 2 * c, other, 1)):
        slot = (zh + step) % 4
        block = ref[k * A_DEV : (k + 1) * A_DEV, :]
        far[pl.ds(pl.multiple_of(slot * A_DEV, A_DEV), A_DEV), :] = block
    tail = pair[2 * A_DEV :, :].astype(F32) + other[2 * A_DEV :, :].astype(F32)
    far[KEYS:, :] = tail.astype(BF16)


def copies_body(line, copies, done):
    moves = [pltpu.make_async_copy(line, copies.at[k], done.at[k]) for k in range(4)]
    for move in moves:
        move.start()
    for move in moves:
        move.wait()


def anchors_body(at, far, ahead, across, behind, anchors):
    row = lax.broadcasted_iota(jnp.int32, (LAB, D), 0)
    tail = jnp.zeros((LAB, D), F32)
    for d, ref in enumerate((far, ahead, across, behind)):
        anchors[d * KEYS : (d + 1) * KEYS, :] = ref[:KEYS, :]
        label = jnp.broadcast_to(ref[KEYS:, :].astype(F32)[:1], (LAB, D))
        tail = jnp.where(row == d, label, tail)
    anchors[4 * KEYS :, :] = tail.astype(BF16)


def label_of(rows):
    rows = rows.astype(F32)
    return rows[:, :KEYS] * 512.0 + rows[:, KEYS : 2 * KEYS]


def scores_of(at, keys_of, rows_of, anchors, first_block, totals, has_own):
    n = KEYS
    labels = label_of(anchors[4 * n :, :])
    if has_own:
        row = lax.broadcasted_iota(jnp.int32, (n, n), 0)
        lane = lax.broadcasted_iota(jnp.int32, (n, n), 1)
        diagonal = (row < A_DEV) & (row + at[0] * A_DEV == lane)
    for half in range(2):
        raw = lax.dot_general(
            keys_of(half),
            anchors[: 4 * n, :],
            (((1,), (1,)), ((), ())),
            preferred_element_type=F32,
        )
        for b in range(2):
            key_label = label_of(rows_of(2 * half + b))[:1]
            key_label = jnp.broadcast_to(key_label, (n, n)).T
            for d in range(4):
                score = raw[b * n : (b + 1) * n, d * n : (d + 1) * n] * 10.0
                expo = jnp.exp(score - 10.0)
                positive = key_label == labels[d : d + 1]
                if has_own and d == 0:
                    itself = diagonal & (at[2] == first_block + 2 * half + b)
                    expo = jnp.where(itself, 0.0, expo)
                    positive = positive & jnp.logical_not(itself)
                parts = (
                    expo,
                    jnp.where(positive, score, 0.0),
                    jnp.where(positive, 1.0, 0.0),
                )
                for k, part in enumerate(parts):
                    totals[d][k] += part.reshape(n // 8, 8, n).sum(axis=0)


def mine_body(at, keys, anchors, out):
    step = pl.program_id(0)

    @pl.when(step == 0)
    def _():
        out[...] = jnp.zeros(out.shape, F32)

    totals = [[out[d, k] for k in range(3)] for d in range(4)]
    scores_of(
        at,
        lambda half: keys[0, 2 * half : 2 * half + 2, :KEYS, :].reshape(2 * KEYS, D),
        lambda block: keys[0, block, KEYS:, :],
        anchors,
        4 * step,
        totals,
        True,
    )
    for d in range(4):
        for k in range(3):
            out[d, k] = totals[d][k]


def theirs_body(at, keys, anchors, before, out):
    totals = [[before[d, k] for k in range(3)] for d in range(4)]
    for p in range(4):
        scores_of(
            at,
            lambda half: keys[p, 2 * half : 2 * half + 2, :KEYS, :].reshape(2 * KEYS, D),
            lambda block: keys[p, block, KEYS:, :],
            anchors,
            4 * p,
            totals,
            False,
        )
    for d in range(4):
        slot = (at[1] + d) % 4
        for k in range(3):
            row = jnp.sum(totals[d][k], axis=0, keepdims=True)
            for z in range(Z):
                out[z, k, pl.ds(slot, 1), :] = row


def loss_body(at, arrived, own, both):
    zh, zl = at[0], at[1]
    total = arrived[0]
    for z in range(1, Z):
        total = total + arrived[z]
    denom, pos_sum, count = total[0], total[1], total[2]
    valid = count > 0.0
    loss = jnp.where(valid, jnp.log(denom) + 10.0 - pos_sum / jnp.maximum(count, 1.0), 0.0)
    classes = lax.broadcasted_iota(jnp.int32, loss.shape, 0)
    mine = jnp.sum(jnp.where(classes == zl, loss, 0.0), axis=0, keepdims=True)
    mine = jnp.broadcast_to(mine, (8, KEYS))
    own[...] = pltpu.roll(mine, (4 - zh) % 4 * A_DEV, 1)
    lane = lax.broadcasted_iota(jnp.int32, (1, KEYS), 1)
    loss_sum = jnp.sum(jnp.sum(loss, axis=0, keepdims=True), axis=1, keepdims=True)
    valid_sum = jnp.sum(
        jnp.sum(jnp.where(valid, 1.0, 0.0), axis=0, keepdims=True), axis=1, keepdims=True
    )
    row = jnp.where(lane == 0, loss_sum, jnp.where(lane == 1, valid_sum, 0.0))
    for k in range(2 * X * Y):
        both[k] = row


def loss_of(embeddings, labels):
    device = lax.axis_index("d")
    c = device % 2
    z = device // 32
    x = device // 4 % 4
    y = device // 16 % 2 * 2 + device // 2 % 2
    own_at = jnp.where(c == 0, y * 4 + x, x * 4 + y)
    at = jnp.stack([z // 4, z % 4, own_at, c]).astype(jnp.int32)

    own_keys, own_anchors = call(
        prepare_body,
        2,
        (jax.ShapeDtypeStruct((4, ROWS, D), BF16), jax.ShapeDtypeStruct((SIDE, D), BF16)),
    )(at, embeddings, labels.reshape(1, KEYS))

    line = swapped_to_all(own_keys, LINES)
    across = along_z(own_anchors, 8)

    copies = pl.pallas_call(
        copies_body,
        name="copies",
        in_specs=[vmem()],
        out_specs=pl.BlockSpec(memory_space=pltpu.HBM),
        out_shape=jax.ShapeDtypeStruct((4, 4, ROWS, D), BF16),
        scratch_shapes=[pltpu.SemaphoreType.DMA((4,))],
        compiler_params=pltpu.CompilerParams(vmem_limit_bytes=50 * 1024 * 1024),
    )(line)
    plane = swapped_to_all(copies, CROSS_LINES)

    two = jax.ShapeDtypeStruct((2 * A_DEV + LAB, D), BF16)
    (pair,) = call(pair_body, 2, (two,))(at, own_anchors, across)
    other_pair = split_along_z(pair, 4)
    (far,) = call(far_body, 2, (jax.ShapeDtypeStruct((ROWS, D), BF16),))(at, pair, other_pair)
    across_near = split_along_z(far, 2)
    behind = along_z(far, 1)
    ahead = along_z(far, -1)

    other_plane = other_core(plane)

    column = jax.ShapeDtypeStruct((4 * KEYS + LAB, D), BF16)
    (anchors,) = call(anchors_body, 4, (column,))(at, far, ahead, across_near, behind)
    whole = lambda dims: pl.BlockSpec(dims, lambda i, at: (0,) * len(dims))
    first = pl.pallas_call(
        mine_body,
        name="mine",
        grid_spec=pltpu.PrefetchScalarGridSpec(
            num_scalar_prefetch=1,
            grid=(4,),
            in_specs=[
                pl.BlockSpec((1, 4, ROWS, D), lambda i, at: (i, 0, 0, 0)),
                whole(column.shape),
            ],
            out_specs=whole((4, 3, 8, KEYS)),
        ),
        out_shape=jax.ShapeDtypeStruct((4, 3, 8, KEYS), F32),
        compiler_params=pltpu.CompilerParams(vmem_limit_bytes=16 * 1024 * 1024),
    )(at, plane, anchors)
    (sums,) = call(
        theirs_body, 3, (jax.ShapeDtypeStruct((Z, 3, 4, KEYS), F32),), (), 16
    )(at, other_plane, anchors, first)
    arrived = swapped_to_all(sums, COLUMNS)
    own_loss, both = call(
        loss_body,
        1,
        (
            jax.ShapeDtypeStruct((8, KEYS), F32),
            jax.ShapeDtypeStruct((2 * X * Y, 1, KEYS), F32),
        ),
    )(at, arrived)
    everyone = swapped_to_all(both, PLANES).sum(axis=0)[0]
    mean_loss = everyone[0] / jnp.maximum(everyone[1], 1.0)
    return (own_loss[0, :A_DEV], mean_loss)


def solution(mesh):
    flat = Mesh(mesh.devices.reshape(512), ("d",))
    placed = (P("d", None), P("d"))
    return jax.shard_map(
        loss_of, mesh=flat, in_specs=placed, out_specs=(P("d"), P()), check_vma=False
    )
```

```python
import jax
import jax.numpy as jnp
from jax import lax
from jax.experimental import pallas as pl
from jax.experimental.pallas import tpu as pltpu
from jax.sharding import Mesh
from jax.sharding import PartitionSpec as P

D = 1024
A_DEV = 32
KEYS = 128
LAB = 8
X = 4
Y = 4
Z = 16
ROWS = KEYS + LAB
SIDE = A_DEV + LAB
F32 = jnp.float32
BF16 = jnp.bfloat16


def device_at(z, x, y, c):
    return ((((z % Z) * 2 + (y % Y) // 2) * X + x % X) * 2 + y % 2) * 2 + c


SPOTS = [(z, x, y, c) for z in range(Z) for x in range(X) for y in range(Y) for c in range(2)]
LINES = [[device_at(z, k, y, 0) for k in range(X)] for z in range(Z) for y in range(Y)] + [
    [device_at(z, x, k, 1) for k in range(Y)] for z in range(Z) for x in range(X)
]
CROSS_LINES = [[device_at(z, x, k, 0) for k in range(Y)] for z in range(Z) for x in range(X)] + [
    [device_at(z, k, y, 1) for k in range(X)] for z in range(Z) for y in range(Y)
]
COLUMNS = [
    [device_at(z, x, y, c) for z in range(Z)] for x in range(X) for y in range(Y) for c in range(2)
]
PLANES = [
    [device_at(z, x, y, c) for x in range(X) for y in range(Y) for c in range(2)] for z in range(Z)
]


def moved(block, target):
    return lax.ppermute(block, "d", [(device_at(*spot), device_at(*target(*spot))) for spot in SPOTS])


def along_z(block, step):
    return moved(block, lambda z, x, y, c: (z + step, x, y, c))


def split_along_z(block, step):
    return moved(block, lambda z, x, y, c: (z + step - 2 * step * c, x, y, c))


def other_core(block):
    return moved(block, lambda z, x, y, c: (z, x, y, 1 - c))


def swapped_to_all(blocks, groups):
    return lax.all_to_all(blocks, "d", 0, 0, tiled=True, axis_index_groups=groups)


def vmem():
    return pl.BlockSpec(memory_space=pltpu.VMEM)


def smem():
    return pl.BlockSpec(memory_space=pltpu.SMEM)


def call(body, n_in, outs, scratch=(), limit=8):
    return pl.pallas_call(
        body,
        in_specs=[smem()] + [vmem()] * n_in,
        out_specs=jax.tree.map(lambda _: vmem(), outs),
        out_shape=outs,
        scratch_shapes=list(scratch),
        compiler_params=pltpu.CompilerParams(vmem_limit_bytes=limit * 1024 * 1024),
    )


def prepare_body(at, emb_in, labels_in, keys_out, anchors, emb, labels, keys, sems):
    ins = [
        pltpu.make_async_copy(emb_in, emb, sems.at[0]),
        pltpu.make_async_copy(labels_in, labels, sems.at[1]),
    ]
    for move in ins:
        move.start()
    ins[1].wait()
    label = jnp.broadcast_to(labels[...], (8, KEYS))
    high = (label + 256) >> 9
    low = label - high * 512
    top = lax.broadcasted_iota(jnp.int32, (8, KEYS), 0) == 0
    lane = lax.broadcasted_iota(jnp.int32, (8, KEYS), 1)
    blank = jnp.zeros((8, D - 2 * KEYS), BF16)
    keys[KEYS:, 2 * KEYS :] = blank
    anchors[A_DEV:, 2 * KEYS :] = blank
    for k, digit in enumerate((high, low)):
        digit = jnp.where(top, digit.astype(F32), 0.0)
        keys[KEYS:, k * KEYS : (k + 1) * KEYS] = digit.astype(BF16)
        mine = pltpu.roll(jnp.where(lane < A_DEV, digit, 0.0), at[0] * A_DEV, 1)
        anchors[A_DEV:, k * KEYS : (k + 1) * KEYS] = mine.astype(BF16)
    ins[0].wait()
    values = emb[...].astype(F32)
    scale = lax.rsqrt(jnp.sum(values * values, axis=1, keepdims=True) + 1e-06)
    unit = (values * scale).astype(BF16)
    keys[:KEYS, :] = unit
    anchors[:A_DEV, :] = unit[:A_DEV]
    outs = [pltpu.make_async_copy(keys, keys_out.at[k], sems.at[2 + k]) for k in range(4)]
    for move in outs:
        move.start()
    for move in outs:
        move.wait()


def pair_body(at, own, across, pair):
    pair[:A_DEV, :] = own[:A_DEV, :]
    pair[A_DEV : 2 * A_DEV, :] = across[:A_DEV, :]
    tail = own[A_DEV:, :].astype(F32) + across[A_DEV:, :].astype(F32)
    pair[2 * A_DEV :, :] = tail.astype(BF16)


def far_body(at, pair, other, far):
    zh, c = at[0], at[3]
    for step, ref, k in ((0, pair, 0), (2, pair, 1), (3 + 2 * c, other, 0), (1 + 2 * c, other, 1)):
        slot = (zh + step) % 4
        block = ref[k * A_DEV : (k + 1) * A_DEV, :]
        far[pl.ds(pl.multiple_of(slot * A_DEV, A_DEV), A_DEV), :] = block
    tail = pair[2 * A_DEV :, :].astype(F32) + other[2 * A_DEV :, :].astype(F32)
    far[KEYS:, :] = tail.astype(BF16)


def copies_body(line, copies, done):
    moves = [pltpu.make_async_copy(line, copies.at[k], done.at[k]) for k in range(4)]
    for move in moves:
        move.start()
    for move in moves:
        move.wait()


def anchors_body(at, far, ahead, across, behind, anchors):
    row = lax.broadcasted_iota(jnp.int32, (LAB, D), 0)
    tail = jnp.zeros((LAB, D), F32)
    for d, ref in enumerate((far, ahead, across, behind)):
        anchors[d * KEYS : (d + 1) * KEYS, :] = ref[:KEYS, :]
        label = jnp.broadcast_to(ref[KEYS:, :].astype(F32)[:1], (LAB, D))
        tail = jnp.where(row == d, label, tail)
    anchors[4 * KEYS :, :] = tail.astype(BF16)


def label_of(rows):
    rows = rows.astype(F32)
    return rows[:, :KEYS] * 512.0 + rows[:, KEYS : 2 * KEYS]


def scores_of(at, keys, anchors, totals, has_own, ready):
    n = KEYS
    labels = label_of(anchors[4 * n :, :])
    if has_own:
        row = lax.broadcasted_iota(jnp.int32, (n, n), 0)
        lane = lax.broadcasted_iota(jnp.int32, (n, n), 1)
        diagonal = (row < A_DEV) & (row + at[0] * A_DEV == lane)

    def product(p, half):
        rows = keys[p, 2 * half : 2 * half + 2, :n, :].reshape(2 * n, D)
        return lax.dot_general(
            rows, anchors[: 4 * n, :], (((1,), (1,)), ((), ())), preferred_element_type=F32
        )

    order = [(p, half) for p in range(4) for half in range(2)]
    ready(0)
    following = product(*order[0])
    for k, (p, half) in enumerate(order):
        raw = following
        if k + 1 < len(order):
            if order[k + 1][1] == 0:
                ready(order[k + 1][0])
            following = product(*order[k + 1])
        for b in range(2):
            key_label = label_of(keys[p, 2 * half + b, n:, :])[:1]
            key_label = jnp.broadcast_to(key_label, (n, n)).T
            for d in range(4):
                dots = raw[b * n : (b + 1) * n, d * n : (d + 1) * n]
                expo = jnp.exp(dots * 10.0 - 10.0)
                positive = key_label == labels[d : d + 1]
                if has_own and d == 0:
                    itself = diagonal & (at[2] == 4 * p + 2 * half + b)
                    expo = jnp.where(itself, 0.0, expo)
                    positive = positive & jnp.logical_not(itself)
                parts = (expo, jnp.where(positive, dots, 0.0), jnp.where(positive, 1.0, 0.0))
                for m, part in enumerate(parts):
                    totals[d][m] += part.reshape(n // 8, 8, n).sum(axis=0)


def mine_body(at, keys_in, anchors, out, keys, sems):
    moves = [pltpu.make_async_copy(keys_in.at[p], keys.at[p], sems.at[p]) for p in range(4)]
    for move in moves:
        move.start()
    totals = [[jnp.zeros((8, KEYS), F32) for _ in range(3)] for _ in range(4)]
    scores_of(at, keys, anchors, totals, True, lambda p: moves[p].wait())
    for d in range(4):
        for k in range(3):
            out[d, k] = totals[d][k]


def theirs_body(at, keys, anchors, before, out):
    totals = [[before[d, k] for k in range(3)] for d in range(4)]
    scores_of(at, keys, anchors, totals, False, lambda p: None)
    for d in range(4):
        slot = (at[1] + d) % 4
        for k in range(3):
            row = jnp.sum(totals[d][k], axis=0, keepdims=True)
            if k == 1:
                row = row * 10.0
            for z in range(Z):
                out[z, k, pl.ds(slot, 1), :] = row


def loss_body(at, arrived, own, both):
    zh, zl = at[0], at[1]
    total = arrived[0]
    for z in range(1, Z):
        total = total + arrived[z]
    denom, pos_sum, count = total[0], total[1], total[2]
    valid = count > 0.0
    loss = jnp.where(valid, jnp.log(denom) + 10.0 - pos_sum / jnp.maximum(count, 1.0), 0.0)
    classes = lax.broadcasted_iota(jnp.int32, loss.shape, 0)
    mine = jnp.sum(jnp.where(classes == zl, loss, 0.0), axis=0, keepdims=True)
    mine = jnp.broadcast_to(mine, (8, KEYS))
    own[...] = pltpu.roll(mine, (4 - zh) % 4 * A_DEV, 1)
    lane = lax.broadcasted_iota(jnp.int32, (1, KEYS), 1)
    loss_sum = jnp.sum(jnp.sum(loss, axis=0, keepdims=True), axis=1, keepdims=True)
    valid_sum = jnp.sum(
        jnp.sum(jnp.where(valid, 1.0, 0.0), axis=0, keepdims=True), axis=1, keepdims=True
    )
    row = jnp.where(lane == 0, loss_sum, jnp.where(lane == 1, valid_sum, 0.0))
    for k in range(2 * X * Y):
        both[k] = row


def loss_of(embeddings, labels):
    device = lax.axis_index("d")
    c = device % 2
    z = device // 32
    x = device // 4 % 4
    y = device // 16 % 2 * 2 + device // 2 % 2
    own_at = jnp.where(c == 0, y * 4 + x, x * 4 + y)
    at = jnp.stack([z // 4, z % 4, own_at, c]).astype(jnp.int32)

    hbm = pl.BlockSpec(memory_space=pltpu.HBM)
    own_keys, own_anchors = pl.pallas_call(
        prepare_body,
        name="prepare",
        in_specs=[smem(), hbm, hbm],
        out_specs=(hbm, vmem()),
        out_shape=(
            jax.ShapeDtypeStruct((4, ROWS, D), BF16),
            jax.ShapeDtypeStruct((SIDE, D), BF16),
        ),
        scratch_shapes=[
            pltpu.VMEM((KEYS, D), BF16),
            pltpu.VMEM((1, KEYS), jnp.int32),
            pltpu.VMEM((ROWS, D), BF16),
            pltpu.SemaphoreType.DMA((6,)),
        ],
        compiler_params=pltpu.CompilerParams(vmem_limit_bytes=54 * 1024 * 1024),
    )(at, embeddings, labels.reshape(1, KEYS))

    line = swapped_to_all(own_keys, LINES)
    across = along_z(own_anchors, 8)

    copies = pl.pallas_call(
        copies_body,
        name="copies",
        in_specs=[vmem()],
        out_specs=pl.BlockSpec(memory_space=pltpu.HBM),
        out_shape=jax.ShapeDtypeStruct((4, 4, ROWS, D), BF16),
        scratch_shapes=[pltpu.SemaphoreType.DMA((4,))],
        compiler_params=pltpu.CompilerParams(vmem_limit_bytes=50 * 1024 * 1024),
    )(line)
    plane = swapped_to_all(copies, CROSS_LINES)

    two = jax.ShapeDtypeStruct((2 * A_DEV + LAB, D), BF16)
    (pair,) = call(pair_body, 2, (two,))(at, own_anchors, across)
    other_pair = split_along_z(pair, 4)
    (far,) = call(far_body, 2, (jax.ShapeDtypeStruct((ROWS, D), BF16),))(at, pair, other_pair)
    across_near = split_along_z(far, 2)
    behind = along_z(far, 1)
    ahead = along_z(far, -1)

    other_plane = other_core(plane)

    column = jax.ShapeDtypeStruct((4 * KEYS + LAB, D), BF16)
    (anchors,) = call(anchors_body, 4, (column,))(at, far, ahead, across_near, behind)
    first = pl.pallas_call(
        mine_body,
        name="mine",
        in_specs=[smem(), hbm, vmem()],
        out_specs=vmem(),
        out_shape=jax.ShapeDtypeStruct((4, 3, 8, KEYS), F32),
        scratch_shapes=[pltpu.VMEM((4, 4, ROWS, D), BF16), pltpu.SemaphoreType.DMA((4,))],
        compiler_params=pltpu.CompilerParams(vmem_limit_bytes=16 * 1024 * 1024),
    )(at, plane, anchors)
    (sums,) = call(
        theirs_body, 3, (jax.ShapeDtypeStruct((Z, 3, 4, KEYS), F32),), (), 16
    )(at, other_plane, anchors, first)
    arrived = swapped_to_all(sums, COLUMNS)
    own_loss, both = call(
        loss_body,
        1,
        (
            jax.ShapeDtypeStruct((8, KEYS), F32),
            jax.ShapeDtypeStruct((2 * X * Y, 1, KEYS), F32),
        ),
    )(at, arrived)
    everyone = swapped_to_all(both, PLANES).sum(axis=0)[0]
    mean_loss = everyone[0] / jnp.maximum(everyone[1], 1.0)
    return (own_loss[0, :A_DEV], mean_loss)


def solution(mesh):
    flat = Mesh(mesh.devices.reshape(512), ("d",))
    placed = (P("d", None), P("d"))
    return jax.shard_map(
        loss_of, mesh=flat, in_specs=placed, out_specs=(P("d"), P()), check_vma=False
    )
```

```python
import jax
import jax.numpy as jnp
from jax import lax
from jax.experimental import pallas as pl
from jax.experimental.pallas import tpu as pltpu
from jax.sharding import Mesh
from jax.sharding import PartitionSpec as P

D = 1024
A_DEV = 32
KEYS = 128
LAB = 8
X = 4
Y = 4
Z = 16
ROWS = KEYS + LAB
SIDE = A_DEV + LAB
F32 = jnp.float32
BF16 = jnp.bfloat16


def device_at(z, x, y, c):
    return ((((z % Z) * 2 + (y % Y) // 2) * X + x % X) * 2 + y % 2) * 2 + c


SPOTS = [(z, x, y, c) for z in range(Z) for x in range(X) for y in range(Y) for c in range(2)]
LINES = [[device_at(z, k, y, 0) for k in range(X)] for z in range(Z) for y in range(Y)] + [
    [device_at(z, x, k, 1) for k in range(Y)] for z in range(Z) for x in range(X)
]
COLUMNS = [
    [device_at(z, x, y, c) for z in range(Z)] for x in range(X) for y in range(Y) for c in range(2)
]
PLANES = [
    [device_at(z, x, y, c) for x in range(X) for y in range(Y) for c in range(2)] for z in range(Z)
]


def moved(block, target):
    return lax.ppermute(block, "d", [(device_at(*spot), device_at(*target(*spot))) for spot in SPOTS])


def along_z(block, step):
    return moved(block, lambda z, x, y, c: (z + step, x, y, c))


def split_along_z(block, step):
    return moved(block, lambda z, x, y, c: (z + step - 2 * step * c, x, y, c))


def across_lines(block, step):
    return moved(
        block, lambda z, x, y, c: (z, x, y + step, c) if c == 0 else (z, x + step, y, c)
    )


def other_core(block):
    return moved(block, lambda z, x, y, c: (z, x, y, 1 - c))


def swapped_to_all(blocks, groups):
    return lax.all_to_all(blocks, "d", 0, 0, tiled=True, axis_index_groups=groups)


def vmem():
    return pl.BlockSpec(memory_space=pltpu.VMEM)


def smem():
    return pl.BlockSpec(memory_space=pltpu.SMEM)


def call(body, n_in, outs, scratch=(), limit=8):
    return pl.pallas_call(
        body,
        in_specs=[smem()] + [vmem()] * n_in,
        out_specs=jax.tree.map(lambda _: vmem(), outs),
        out_shape=outs,
        scratch_shapes=list(scratch),
        compiler_params=pltpu.CompilerParams(vmem_limit_bytes=limit * 1024 * 1024),
    )


def prepare_body(at, emb, labels, keys, anchors):
    values = emb[...].astype(F32)
    scale = lax.rsqrt(jnp.sum(values * values, axis=1, keepdims=True) + 1e-06)
    unit = (values * scale).astype(BF16)
    for k in range(4):
        keys[k, :KEYS, :] = unit
    anchors[:A_DEV, :] = unit[:A_DEV]
    label = jnp.broadcast_to(labels[...], (8, KEYS))
    high = (label + 256) >> 9
    low = label - high * 512
    top = lax.broadcasted_iota(jnp.int32, (8, KEYS), 0) == 0
    lane = lax.broadcasted_iota(jnp.int32, (8, KEYS), 1)
    blank = jnp.zeros((8, D - 2 * KEYS), BF16)
    for k in range(4):
        keys[k, KEYS:, 2 * KEYS :] = blank
    anchors[A_DEV:, 2 * KEYS :] = blank
    for k, digit in enumerate((high, low)):
        digit = jnp.where(top, digit.astype(F32), 0.0)
        for copy in range(4):
            keys[copy, KEYS:, k * KEYS : (k + 1) * KEYS] = digit.astype(BF16)
        mine = pltpu.roll(jnp.where(lane < A_DEV, digit, 0.0), at[0] * A_DEV, 1)
        anchors[A_DEV:, k * KEYS : (k + 1) * KEYS] = mine.astype(BF16)


def pair_body(at, own, across, pair):
    pair[:A_DEV, :] = own[:A_DEV, :]
    pair[A_DEV : 2 * A_DEV, :] = across[:A_DEV, :]
    tail = own[A_DEV:, :].astype(F32) + across[A_DEV:, :].astype(F32)
    pair[2 * A_DEV :, :] = tail.astype(BF16)


def far_body(at, pair, other, far):
    zh, c = at[0], at[3]
    for step, ref, k in ((0, pair, 0), (2, pair, 1), (3 + 2 * c, other, 0), (1 + 2 * c, other, 1)):
        slot = (zh + step) % 4
        block = ref[k * A_DEV : (k + 1) * A_DEV, :]
        far[pl.ds(pl.multiple_of(slot * A_DEV, A_DEV), A_DEV), :] = block
    tail = pair[2 * A_DEV :, :].astype(F32) + other[2 * A_DEV :, :].astype(F32)
    far[KEYS:, :] = tail.astype(BF16)


def anchors_body(at, far, ahead, across, behind, anchors):
    row = lax.broadcasted_iota(jnp.int32, (LAB, D), 0)
    tail = jnp.zeros((LAB, D), F32)
    for d, ref in enumerate((far, ahead, across, behind)):
        anchors[d * KEYS : (d + 1) * KEYS, :] = ref[:KEYS, :]
        label = jnp.broadcast_to(ref[KEYS:, :].astype(F32)[:1], (LAB, D))
        tail = jnp.where(row == d, label, tail)
    anchors[4 * KEYS :, :] = tail.astype(BF16)


def label_of(rows):
    rows = rows.astype(F32)
    return rows[:, :KEYS] * 512.0 + rows[:, KEYS : 2 * KEYS]


def scores_of(at, keys, anchors, totals, has_own):
    n = KEYS
    labels = label_of(anchors[4 * n :, :])
    if has_own:
        row = lax.broadcasted_iota(jnp.int32, (n, n), 0)
        lane = lax.broadcasted_iota(jnp.int32, (n, n), 1)
        diagonal = (row < A_DEV) & (row + at[0] * A_DEV == lane)

    def product(p, half):
        rows = keys[p][2 * half : 2 * half + 2, :n, :].reshape(2 * n, D)
        return lax.dot_general(
            rows, anchors[: 4 * n, :], (((1,), (1,)), ((), ())), preferred_element_type=F32
        )

    order = [(p, half) for p in range(4) for half in range(2)]
    following = product(*order[0])
    for k, (p, half) in enumerate(order):
        raw = following
        if k + 1 < len(order):
            following = product(*order[k + 1])
        for b in range(2):
            key_label = label_of(keys[p][2 * half + b, n:, :])[:1]
            key_label = jnp.broadcast_to(key_label, (n, n)).T
            for d in range(4):
                dots = raw[b * n : (b + 1) * n, d * n : (d + 1) * n]
                expo = jnp.exp(dots * 10.0 - 10.0)
                positive = key_label == labels[d : d + 1]
                if has_own and p == 0 and d == 0:
                    itself = diagonal & (at[2] == 2 * half + b)
                    expo = jnp.where(itself, 0.0, expo)
                    positive = positive & jnp.logical_not(itself)
                parts = (expo, jnp.where(positive, dots, 0.0), jnp.where(positive, 1.0, 0.0))
                for m, part in enumerate(parts):
                    totals[d][m] += part.reshape(n // 8, 8, n).sum(axis=0)


def mine_body(at, line, plus, minus, two, anchors, out):
    totals = [[jnp.zeros((8, KEYS), F32) for _ in range(3)] for _ in range(4)]
    scores_of(at, (line, plus, minus, two), anchors, totals, True)
    for d in range(4):
        for k in range(3):
            out[d, k] = totals[d][k]


def theirs_body(at, line, plus, minus, two, anchors, before, out):
    totals = [[before[d, k] for k in range(3)] for d in range(4)]
    scores_of(at, (line, plus, minus, two), anchors, totals, False)
    for d in range(4):
        slot = (at[1] + d) % 4
        for k in range(3):
            row = jnp.sum(totals[d][k], axis=0, keepdims=True)
            if k == 1:
                row = row * 10.0
            for z in range(Z):
                out[z, k, pl.ds(slot, 1), :] = row


def loss_body(at, arrived, own, both):
    zh, zl = at[0], at[1]
    total = arrived[0]
    for z in range(1, Z):
        total = total + arrived[z]
    denom, pos_sum, count = total[0], total[1], total[2]
    valid = count > 0.0
    loss = jnp.where(valid, jnp.log(denom) + 10.0 - pos_sum / jnp.maximum(count, 1.0), 0.0)
    classes = lax.broadcasted_iota(jnp.int32, loss.shape, 0)
    mine = jnp.sum(jnp.where(classes == zl, loss, 0.0), axis=0, keepdims=True)
    mine = jnp.broadcast_to(mine, (8, KEYS))
    own[...] = pltpu.roll(mine, (4 - zh) % 4 * A_DEV, 1)
    lane = lax.broadcasted_iota(jnp.int32, (1, KEYS), 1)
    loss_sum = jnp.sum(jnp.sum(loss, axis=0, keepdims=True), axis=1, keepdims=True)
    valid_sum = jnp.sum(
        jnp.sum(jnp.where(valid, 1.0, 0.0), axis=0, keepdims=True), axis=1, keepdims=True
    )
    row = jnp.where(lane == 0, loss_sum, jnp.where(lane == 1, valid_sum, 0.0))
    for k in range(2 * X * Y):
        both[k] = row


def loss_of(embeddings, labels):
    device = lax.axis_index("d")
    c = device % 2
    z = device // 32
    x = device // 4 % 4
    y = device // 16 % 2 * 2 + device // 2 % 2
    at = jnp.stack([z // 4, z % 4, jnp.where(c == 0, x, y), c]).astype(jnp.int32)

    own_keys, own_anchors = call(
        prepare_body,
        2,
        (jax.ShapeDtypeStruct((4, ROWS, D), BF16), jax.ShapeDtypeStruct((SIDE, D), BF16)),
    )(at, embeddings, labels.reshape(1, KEYS))

    line = swapped_to_all(own_keys, LINES)
    across = along_z(own_anchors, 8)

    mine = [line]
    for step in (1, -1, 2):
        mine.append(across_lines(line, step))

    two = jax.ShapeDtypeStruct((2 * A_DEV + LAB, D), BF16)
    (pair,) = call(pair_body, 2, (two,))(at, own_anchors, across)
    other_pair = split_along_z(pair, 4)
    (far,) = call(far_body, 2, (jax.ShapeDtypeStruct((ROWS, D), BF16),))(at, pair, other_pair)
    across_near = split_along_z(far, 2)
    behind = along_z(far, 1)
    ahead = along_z(far, -1)

    theirs = []
    for block in mine:
        theirs.append(other_core(block))

    column = jax.ShapeDtypeStruct((4 * KEYS + LAB, D), BF16)
    (anchors,) = call(anchors_body, 4, (column,))(at, far, ahead, across_near, behind)
    (first,) = call(mine_body, 5, (jax.ShapeDtypeStruct((4, 3, 8, KEYS), F32),), (), 16)(
        at, *mine, anchors
    )
    (sums,) = call(
        theirs_body, 6, (jax.ShapeDtypeStruct((Z, 3, 4, KEYS), F32),), (), 16
    )(at, *theirs, anchors, first)
    arrived = swapped_to_all(sums, COLUMNS)
    own_loss, both = call(
        loss_body,
        1,
        (
            jax.ShapeDtypeStruct((8, KEYS), F32),
            jax.ShapeDtypeStruct((2 * X * Y, 1, KEYS), F32),
        ),
    )(at, arrived)
    everyone = swapped_to_all(both, PLANES).sum(axis=0)[0]
    mean_loss = everyone[0] / jnp.maximum(everyone[1], 1.0)
    return (own_loss[0, :A_DEV], mean_loss)


def solution(mesh):
    flat = Mesh(mesh.devices.reshape(512), ("d",))
    placed = (P("d", None), P("d"))
    return jax.shard_map(
        loss_of, mesh=flat, in_specs=placed, out_specs=(P("d"), P()), check_vma=False
    )
```

```python
import jax
import jax.numpy as jnp
from jax import lax
from jax.experimental import pallas as pl
from jax.experimental.pallas import tpu as pltpu
from jax.sharding import Mesh
from jax.sharding import PartitionSpec as P

D = 1024
A_DEV = 32
KEYS = 128
LAB = 8
X = 4
Y = 4
Z = 16
ROWS = KEYS + LAB
SIDE = A_DEV + LAB
F32 = jnp.float32
BF16 = jnp.bfloat16


def device_at(z, x, y, c):
    return ((((z % Z) * 2 + (y % Y) // 2) * X + x % X) * 2 + y % 2) * 2 + c


SPOTS = [(z, x, y, c) for z in range(Z) for x in range(X) for y in range(Y) for c in range(2)]
LINES = [[device_at(z, k, y, 0) for k in range(X)] for z in range(Z) for y in range(Y)] + [
    [device_at(z, x, k, 1) for k in range(Y)] for z in range(Z) for x in range(X)
]
COLUMNS = [
    [device_at(z, x, y, c) for z in range(Z)] for x in range(X) for y in range(Y) for c in range(2)
]
PLANES = [
    [device_at(z, x, y, c) for x in range(X) for y in range(Y) for c in range(2)] for z in range(Z)
]


def moved(block, target):
    return lax.ppermute(block, "d", [(device_at(*spot), device_at(*target(*spot))) for spot in SPOTS])


def along_z(block, step):
    return moved(block, lambda z, x, y, c: (z + step, x, y, c))


def split_along_z(block, step):
    return moved(block, lambda z, x, y, c: (z + step - 2 * step * c, x, y, c))


def across_lines(block, step):
    return moved(
        block, lambda z, x, y, c: (z, x, y + step, c) if c == 0 else (z, x + step, y, c)
    )


def other_core(block):
    return moved(block, lambda z, x, y, c: (z, x, y, 1 - c))


def swapped_to_all(blocks, groups):
    return lax.all_to_all(blocks, "d", 0, 0, tiled=True, axis_index_groups=groups)


def vmem():
    return pl.BlockSpec(memory_space=pltpu.VMEM)


def smem():
    return pl.BlockSpec(memory_space=pltpu.SMEM)


def call(body, n_in, outs, scratch=(), limit=8):
    return pl.pallas_call(
        body,
        in_specs=[smem()] + [vmem()] * n_in,
        out_specs=jax.tree.map(lambda _: vmem(), outs),
        out_shape=outs,
        scratch_shapes=list(scratch),
        compiler_params=pltpu.CompilerParams(vmem_limit_bytes=limit * 1024 * 1024),
    )


def prepare_body(at, emb, labels, keys, anchors):
    values = emb[...].astype(F32)
    scale = lax.rsqrt(jnp.sum(values * values, axis=1, keepdims=True) + 1e-06)
    unit = (values * scale).astype(BF16)
    for k in range(4):
        keys[k, :KEYS, :] = unit
    anchors[:A_DEV, :] = unit[:A_DEV]
    label = jnp.broadcast_to(labels[...], (8, KEYS))
    high = (label + 256) >> 9
    low = label - high * 512
    top = lax.broadcasted_iota(jnp.int32, (8, KEYS), 0) == 0
    lane = lax.broadcasted_iota(jnp.int32, (8, KEYS), 1)
    blank = jnp.zeros((8, D - 2 * KEYS), BF16)
    for k in range(4):
        keys[k, KEYS:, 2 * KEYS :] = blank
    anchors[A_DEV:, 2 * KEYS :] = blank
    for k, digit in enumerate((high, low)):
        digit = jnp.where(top, digit.astype(F32), 0.0)
        for copy in range(4):
            keys[copy, KEYS:, k * KEYS : (k + 1) * KEYS] = digit.astype(BF16)
        mine = pltpu.roll(jnp.where(lane < A_DEV, digit, 0.0), at[0] * A_DEV, 1)
        anchors[A_DEV:, k * KEYS : (k + 1) * KEYS] = mine.astype(BF16)


def pair_body(at, own, across, pair):
    pair[:A_DEV, :] = own[:A_DEV, :]
    pair[A_DEV : 2 * A_DEV, :] = across[:A_DEV, :]
    tail = own[A_DEV:, :].astype(F32) + across[A_DEV:, :].astype(F32)
    pair[2 * A_DEV :, :] = tail.astype(BF16)


def far_body(at, pair, other, far):
    zh, c = at[0], at[3]
    for step, ref, k in ((0, pair, 0), (2, pair, 1), (3 + 2 * c, other, 0), (1 + 2 * c, other, 1)):
        slot = (zh + step) % 4
        block = ref[k * A_DEV : (k + 1) * A_DEV, :]
        far[pl.ds(pl.multiple_of(slot * A_DEV, A_DEV), A_DEV), :] = block
    tail = pair[2 * A_DEV :, :].astype(F32) + other[2 * A_DEV :, :].astype(F32)
    far[KEYS:, :] = tail.astype(BF16)


def rest_body(at, plus, minus, two, rest):
    for k, ref in enumerate((plus, minus, two)):
        rest[k] = ref[...]


def anchors_body(at, far, ahead, across, behind, anchors):
    row = lax.broadcasted_iota(jnp.int32, (LAB, D), 0)
    tail = jnp.zeros((LAB, D), F32)
    for d, ref in enumerate((far, ahead, across, behind)):
        anchors[d * KEYS : (d + 1) * KEYS, :] = ref[:KEYS, :]
        label = jnp.broadcast_to(ref[KEYS:, :].astype(F32)[:1], (LAB, D))
        tail = jnp.where(row == d, label, tail)
    anchors[4 * KEYS :, :] = tail.astype(BF16)


def label_of(rows):
    rows = rows.astype(F32)
    return rows[:, :KEYS] * 512.0 + rows[:, KEYS : 2 * KEYS]


def scores_of(at, keys, anchors, totals, has_own):
    n = KEYS
    labels = label_of(anchors[4 * n :, :])
    if has_own:
        row = lax.broadcasted_iota(jnp.int32, (n, n), 0)
        lane = lax.broadcasted_iota(jnp.int32, (n, n), 1)
        diagonal = (row < A_DEV) & (row + at[0] * A_DEV == lane)

    def product(p, half):
        rows = keys[p][2 * half : 2 * half + 2, :n, :].reshape(2 * n, D)
        return lax.dot_general(
            rows, anchors[: 4 * n, :], (((1,), (1,)), ((), ())), preferred_element_type=F32
        )

    order = [(p, half) for p in range(4) for half in range(2)]
    following = product(*order[0])
    for k, (p, half) in enumerate(order):
        raw = following
        if k + 1 < len(order):
            following = product(*order[k + 1])
        for b in range(2):
            key_label = label_of(keys[p][2 * half + b, n:, :])[:1]
            key_label = jnp.broadcast_to(key_label, (n, n)).T
            for d in range(4):
                dots = raw[b * n : (b + 1) * n, d * n : (d + 1) * n]
                expo = jnp.exp(dots * 10.0 - 10.0)
                positive = key_label == labels[d : d + 1]
                if has_own and p == 0 and d == 0:
                    itself = diagonal & (at[2] == 2 * half + b)
                    expo = jnp.where(itself, 0.0, expo)
                    positive = positive & jnp.logical_not(itself)
                parts = (expo, jnp.where(positive, dots, 0.0), jnp.where(positive, 1.0, 0.0))
                for m, part in enumerate(parts):
                    totals[d][m] += part.reshape(n // 8, 8, n).sum(axis=0)


def mine_body(at, line, rest, anchors, out):
    totals = [[jnp.zeros((8, KEYS), F32) for _ in range(3)] for _ in range(4)]
    scores_of(at, (line, rest.at[0], rest.at[1], rest.at[2]), anchors, totals, True)
    for d in range(4):
        for k in range(3):
            out[d, k] = totals[d][k]


def theirs_body(at, line, rest, anchors, before, out):
    totals = [[before[d, k] for k in range(3)] for d in range(4)]
    scores_of(at, (line, rest.at[0], rest.at[1], rest.at[2]), anchors, totals, False)
    for d in range(4):
        slot = (at[1] + d) % 4
        for k in range(3):
            row = jnp.sum(totals[d][k], axis=0, keepdims=True)
            if k == 1:
                row = row * 10.0
            for z in range(Z):
                out[z, k, pl.ds(slot, 1), :] = row


def loss_body(at, arrived, own, both):
    zh, zl = at[0], at[1]
    total = arrived[0]
    for z in range(1, Z):
        total = total + arrived[z]
    denom, pos_sum, count = total[0], total[1], total[2]
    valid = count > 0.0
    loss = jnp.where(valid, jnp.log(denom) + 10.0 - pos_sum / jnp.maximum(count, 1.0), 0.0)
    classes = lax.broadcasted_iota(jnp.int32, loss.shape, 0)
    mine = jnp.sum(jnp.where(classes == zl, loss, 0.0), axis=0, keepdims=True)
    mine = jnp.broadcast_to(mine, (8, KEYS))
    own[...] = pltpu.roll(mine, (4 - zh) % 4 * A_DEV, 1)
    lane = lax.broadcasted_iota(jnp.int32, (1, KEYS), 1)
    loss_sum = jnp.sum(jnp.sum(loss, axis=0, keepdims=True), axis=1, keepdims=True)
    valid_sum = jnp.sum(
        jnp.sum(jnp.where(valid, 1.0, 0.0), axis=0, keepdims=True), axis=1, keepdims=True
    )
    row = jnp.where(lane == 0, loss_sum, jnp.where(lane == 1, valid_sum, 0.0))
    for k in range(2 * X * Y):
        both[k] = row


def loss_of(embeddings, labels):
    device = lax.axis_index("d")
    c = device % 2
    z = device // 32
    x = device // 4 % 4
    y = device // 16 % 2 * 2 + device // 2 % 2
    at = jnp.stack([z // 4, z % 4, jnp.where(c == 0, x, y), c]).astype(jnp.int32)

    own_keys, own_anchors = call(
        prepare_body,
        2,
        (jax.ShapeDtypeStruct((4, ROWS, D), BF16), jax.ShapeDtypeStruct((SIDE, D), BF16)),
    )(at, embeddings, labels.reshape(1, KEYS))

    line = swapped_to_all(own_keys, LINES)
    across = along_z(own_anchors, 8)

    plane = []
    for step in (1, -1, 2):
        plane.append(across_lines(line, step))

    two = jax.ShapeDtypeStruct((2 * A_DEV + LAB, D), BF16)
    (pair,) = call(pair_body, 2, (two,))(at, own_anchors, across)
    other_pair = split_along_z(pair, 4)
    (far,) = call(far_body, 2, (jax.ShapeDtypeStruct((ROWS, D), BF16),))(at, pair, other_pair)
    across_near = split_along_z(far, 2)
    behind = along_z(far, 1)
    ahead = along_z(far, -1)

    (rest,) = call(rest_body, 3, (jax.ShapeDtypeStruct((3, 4, ROWS, D), BF16),))(at, *plane)
    other_line = other_core(line)
    other_rest = other_core(rest)

    column = jax.ShapeDtypeStruct((4 * KEYS + LAB, D), BF16)
    (anchors,) = call(anchors_body, 4, (column,))(at, far, ahead, across_near, behind)
    (first,) = call(mine_body, 3, (jax.ShapeDtypeStruct((4, 3, 8, KEYS), F32),), (), 16)(
        at, line, rest, anchors
    )
    (sums,) = call(
        theirs_body, 4, (jax.ShapeDtypeStruct((Z, 3, 4, KEYS), F32),), (), 16
    )(at, other_line, other_rest, anchors, first)
    arrived = swapped_to_all(sums, COLUMNS)
    own_loss, both = call(
        loss_body,
        1,
        (
            jax.ShapeDtypeStruct((8, KEYS), F32),
            jax.ShapeDtypeStruct((2 * X * Y, 1, KEYS), F32),
        ),
    )(at, arrived)
    anchor_loss, both = lax.optimization_barrier((own_loss[0, :A_DEV], both))
    everyone = swapped_to_all(both, PLANES).sum(axis=0)[0]
    mean_loss = everyone[0] / jnp.maximum(everyone[1], 1.0)
    return (anchor_loss, mean_loss)


def solution(mesh):
    flat = Mesh(mesh.devices.reshape(512), ("d",))
    placed = (P("d", None), P("d"))
    return jax.shard_map(
        loss_of, mesh=flat, in_specs=placed, out_specs=(P("d"), P()), check_vma=False
    )
```

```python
import jax
import jax.numpy as jnp
from jax import lax
from jax.experimental import pallas as pl
from jax.experimental.pallas import tpu as pltpu
from jax.sharding import Mesh
from jax.sharding import PartitionSpec as P

D = 1024
A_DEV = 32
KEYS = 128
LAB = 8
X = 4
Y = 4
Z = 16
ROWS = KEYS + LAB
SIDE = A_DEV + LAB
F32 = jnp.float32
BF16 = jnp.bfloat16


def device_at(z, x, y, c):
    return ((((z % Z) * 2 + (y % Y) // 2) * X + x % X) * 2 + y % 2) * 2 + c


SPOTS = [(z, x, y, c) for z in range(Z) for x in range(X) for y in range(Y) for c in range(2)]
LINES = [[device_at(z, k, y, 0) for k in range(X)] for z in range(Z) for y in range(Y)] + [
    [device_at(z, x, k, 1) for k in range(Y)] for z in range(Z) for x in range(X)
]
COLUMNS = [
    [device_at(z, x, y, c) for z in range(Z)] for x in range(X) for y in range(Y) for c in range(2)
]
PLANES = [
    [device_at(z, x, y, c) for x in range(X) for y in range(Y) for c in range(2)] for z in range(Z)
]


def moved(block, target):
    return lax.ppermute(block, "d", [(device_at(*spot), device_at(*target(*spot))) for spot in SPOTS])


def along_z(block, step):
    return moved(block, lambda z, x, y, c: (z + step, x, y, c))


def split_along_z(block, step):
    return moved(block, lambda z, x, y, c: (z + step - 2 * step * c, x, y, c))


def across_lines(block, step):
    return moved(
        block, lambda z, x, y, c: (z, x, y + step, c) if c == 0 else (z, x + step, y, c)
    )


def other_core(block):
    return moved(block, lambda z, x, y, c: (z, x, y, 1 - c))


def swapped_to_all(blocks, groups):
    return lax.all_to_all(blocks, "d", 0, 0, tiled=True, axis_index_groups=groups)


def vmem():
    return pl.BlockSpec(memory_space=pltpu.VMEM)


def smem():
    return pl.BlockSpec(memory_space=pltpu.SMEM)


def call(body, n_in, outs, scratch=(), limit=8):
    return pl.pallas_call(
        body,
        in_specs=[smem()] + [vmem()] * n_in,
        out_specs=jax.tree.map(lambda _: vmem(), outs),
        out_shape=outs,
        scratch_shapes=list(scratch),
        compiler_params=pltpu.CompilerParams(vmem_limit_bytes=limit * 1024 * 1024),
    )


def prepare_body(at, emb, labels, keys, anchors):
    values = emb[...].astype(F32)
    scale = lax.rsqrt(jnp.sum(values * values, axis=1, keepdims=True) + 1e-06)
    unit = (values * scale).astype(BF16)
    for k in range(4):
        keys[k, :KEYS, :] = unit
    anchors[:A_DEV, :] = unit[:A_DEV]
    label = jnp.broadcast_to(labels[...], (8, KEYS))
    high = (label + 256) >> 9
    low = label - high * 512
    top = lax.broadcasted_iota(jnp.int32, (8, KEYS), 0) == 0
    lane = lax.broadcasted_iota(jnp.int32, (8, KEYS), 1)
    blank = jnp.zeros((8, D - 2 * KEYS), BF16)
    for k in range(4):
        keys[k, KEYS:, 2 * KEYS :] = blank
    anchors[A_DEV:, 2 * KEYS :] = blank
    for k, digit in enumerate((high, low)):
        digit = jnp.where(top, digit.astype(F32), 0.0)
        for copy in range(4):
            keys[copy, KEYS:, k * KEYS : (k + 1) * KEYS] = digit.astype(BF16)
        mine = pltpu.roll(jnp.where(lane < A_DEV, digit, 0.0), at[0] * A_DEV, 1)
        anchors[A_DEV:, k * KEYS : (k + 1) * KEYS] = mine.astype(BF16)


def pair_body(at, own, across, pair):
    pair[:A_DEV, :] = own[:A_DEV, :]
    pair[A_DEV : 2 * A_DEV, :] = across[:A_DEV, :]
    tail = own[A_DEV:, :].astype(F32) + across[A_DEV:, :].astype(F32)
    pair[2 * A_DEV :, :] = tail.astype(BF16)


def far_body(at, pair, other, far):
    zh, c = at[0], at[3]
    for step, ref, k in ((0, pair, 0), (2, pair, 1), (3 + 2 * c, other, 0), (1 + 2 * c, other, 1)):
        slot = (zh + step) % 4
        block = ref[k * A_DEV : (k + 1) * A_DEV, :]
        far[pl.ds(pl.multiple_of(slot * A_DEV, A_DEV), A_DEV), :] = block
    tail = pair[2 * A_DEV :, :].astype(F32) + other[2 * A_DEV :, :].astype(F32)
    far[KEYS:, :] = tail.astype(BF16)


def rest_body(at, plus, minus, two, rest):
    for k, ref in enumerate((plus, minus, two)):
        rest[k] = ref[...]


def anchors_body(at, far, ahead, across, behind, anchors):
    row = lax.broadcasted_iota(jnp.int32, (LAB, D), 0)
    tail = jnp.zeros((LAB, D), F32)
    for d, ref in enumerate((far, ahead, across, behind)):
        anchors[d * KEYS : (d + 1) * KEYS, :] = ref[:KEYS, :]
        label = jnp.broadcast_to(ref[KEYS:, :].astype(F32)[:1], (LAB, D))
        tail = jnp.where(row == d, label, tail)
    anchors[4 * KEYS :, :] = tail.astype(BF16)


def label_of(rows):
    rows = rows.astype(F32)
    return rows[:, :KEYS] * 512.0 + rows[:, KEYS : 2 * KEYS]


def scores_of(at, keys, anchors, totals, has_own):
    n = KEYS
    labels = label_of(anchors[4 * n :, :])
    if has_own:
        row = lax.broadcasted_iota(jnp.int32, (n, n), 0)
        lane = lax.broadcasted_iota(jnp.int32, (n, n), 1)
        diagonal = (row < A_DEV) & (row + at[0] * A_DEV == lane)

    def product(p, half):
        rows = keys[p][2 * half : 2 * half + 2, :n, :].reshape(2 * n, D)
        return lax.dot_general(
            rows, anchors[: 4 * n, :], (((1,), (1,)), ((), ())), preferred_element_type=F32
        )

    order = [(p, half) for p in range(4) for half in range(2)]
    following = product(*order[0])
    for k, (p, half) in enumerate(order):
        raw = following
        if k + 1 < len(order):
            following = product(*order[k + 1])
        for b in range(2):
            key_label = label_of(keys[p][2 * half + b, n:, :])[:1]
            key_label = jnp.broadcast_to(key_label, (n, n)).T
            for d in range(4):
                dots = raw[b * n : (b + 1) * n, d * n : (d + 1) * n]
                expo = jnp.exp(dots * 10.0 - 10.0)
                positive = key_label == labels[d : d + 1]
                if has_own and p == 0 and d == 0:
                    itself = diagonal & (at[2] == 2 * half + b)
                    expo = jnp.where(itself, 0.0, expo)
                    positive = positive & jnp.logical_not(itself)
                parts = (expo, jnp.where(positive, dots, 0.0), jnp.where(positive, 1.0, 0.0))
                for m, part in enumerate(parts):
                    totals[d][m] += part.reshape(n // 8, 8, n).sum(axis=0)


def mine_body(at, line, rest, anchors, out):
    totals = [[jnp.zeros((8, KEYS), F32) for _ in range(3)] for _ in range(4)]
    scores_of(at, (line, rest.at[0], rest.at[1], rest.at[2]), anchors, totals, True)
    for d in range(4):
        for k in range(3):
            out[d, k] = totals[d][k]


def theirs_body(at, line, rest, anchors, before, out):
    totals = [[before[d, k] for k in range(3)] for d in range(4)]
    scores_of(at, (line, rest.at[0], rest.at[1], rest.at[2]), anchors, totals, False)
    for d in range(4):
        slot = (at[1] + d) % 4
        for k in range(3):
            row = jnp.sum(totals[d][k], axis=0, keepdims=True)
            if k == 1:
                row = row * 10.0
            for z in range(Z):
                out[z, k, pl.ds(slot, 1), :] = row


def loss_body(at, arrived, own, both):
    zh, zl = at[0], at[1]
    total = arrived[0]
    for z in range(1, Z):
        total = total + arrived[z]
    denom, pos_sum, count = total[0], total[1], total[2]
    valid = count > 0.0
    loss = jnp.where(valid, jnp.log(denom) + 10.0 - pos_sum / jnp.maximum(count, 1.0), 0.0)
    classes = lax.broadcasted_iota(jnp.int32, loss.shape, 0)
    mine = jnp.sum(jnp.where(classes == zl, loss, 0.0), axis=0, keepdims=True)
    mine = jnp.broadcast_to(mine, (8, KEYS))
    own[...] = pltpu.roll(mine, (4 - zh) % 4 * A_DEV, 1)[0, :A_DEV]
    lane = lax.broadcasted_iota(jnp.int32, (1, KEYS), 1)
    loss_sum = jnp.sum(jnp.sum(loss, axis=0, keepdims=True), axis=1, keepdims=True)
    valid_sum = jnp.sum(
        jnp.sum(jnp.where(valid, 1.0, 0.0), axis=0, keepdims=True), axis=1, keepdims=True
    )
    row = jnp.where(lane == 0, loss_sum, jnp.where(lane == 1, valid_sum, 0.0))
    for k in range(2 * X * Y):
        both[k] = row


def loss_of(embeddings, labels):
    device = lax.axis_index("d")
    c = device % 2
    z = device // 32
    x = device // 4 % 4
    y = device // 16 % 2 * 2 + device // 2 % 2
    at = jnp.stack([z // 4, z % 4, jnp.where(c == 0, x, y), c]).astype(jnp.int32)

    own_keys, own_anchors = call(
        prepare_body,
        2,
        (jax.ShapeDtypeStruct((4, ROWS, D), BF16), jax.ShapeDtypeStruct((SIDE, D), BF16)),
    )(at, embeddings, labels.reshape(1, KEYS))

    line = swapped_to_all(own_keys, LINES)
    across = along_z(own_anchors, 8)

    plane = []
    for step in (1, -1, 2):
        plane.append(across_lines(line, step))

    two = jax.ShapeDtypeStruct((2 * A_DEV + LAB, D), BF16)
    (pair,) = call(pair_body, 2, (two,))(at, own_anchors, across)
    other_pair = split_along_z(pair, 4)
    (far,) = call(far_body, 2, (jax.ShapeDtypeStruct((ROWS, D), BF16),))(at, pair, other_pair)
    across_near = split_along_z(far, 2)
    behind = along_z(far, 1)
    ahead = along_z(far, -1)

    (rest,) = call(rest_body, 3, (jax.ShapeDtypeStruct((3, 4, ROWS, D), BF16),))(at, *plane)
    other_line = other_core(line)
    other_rest = other_core(rest)

    column = jax.ShapeDtypeStruct((4 * KEYS + LAB, D), BF16)
    (anchors,) = call(anchors_body, 4, (column,))(at, far, ahead, across_near, behind)
    (first,) = call(mine_body, 3, (jax.ShapeDtypeStruct((4, 3, 8, KEYS), F32),), (), 16)(
        at, line, rest, anchors
    )
    (sums,) = call(
        theirs_body, 4, (jax.ShapeDtypeStruct((Z, 3, 4, KEYS), F32),), (), 16
    )(at, other_line, other_rest, anchors, first)
    arrived = swapped_to_all(sums, COLUMNS)
    own_loss, both = call(
        loss_body,
        1,
        (
            jax.ShapeDtypeStruct((A_DEV,), F32),
            jax.ShapeDtypeStruct((2 * X * Y, 1, KEYS), F32),
        ),
    )(at, arrived)
    anchor_loss, both = lax.optimization_barrier((own_loss, both))
    everyone = swapped_to_all(both, PLANES).sum(axis=0)[0]
    mean_loss = everyone[0] / jnp.maximum(everyone[1], 1.0)
    return (anchor_loss, mean_loss)


def solution(mesh):
    flat = Mesh(mesh.devices.reshape(512), ("d",))
    placed = (P("d", None), P("d"))
    return jax.shard_map(
        loss_of, mesh=flat, in_specs=placed, out_specs=(P("d"), P()), check_vma=False
    )
```

```python
import jax
import jax.numpy as jnp
from jax import lax
from jax.experimental import pallas as pl
from jax.experimental.pallas import tpu as pltpu
from jax.sharding import Mesh
from jax.sharding import PartitionSpec as P

D = 1024
A_DEV = 32
KEYS = 128
LAB = 8
X = 4
Y = 4
Z = 16
ROWS = KEYS + LAB
SIDE = A_DEV + LAB
F32 = jnp.float32
BF16 = jnp.bfloat16


def device_at(z, x, y, c):
    return ((((z % Z) * 2 + (y % Y) // 2) * X + x % X) * 2 + y % 2) * 2 + c


SPOTS = [(z, x, y, c) for z in range(Z) for x in range(X) for y in range(Y) for c in range(2)]
LINES = [[device_at(z, k, y, 0) for k in range(X)] for z in range(Z) for y in range(Y)] + [
    [device_at(z, x, k, 1) for k in range(Y)] for z in range(Z) for x in range(X)
]
COLUMNS = [
    [device_at(z, x, y, c) for z in range(Z)] for x in range(X) for y in range(Y) for c in range(2)
]
PLANES = [
    [device_at(z, x, y, c) for x in range(X) for y in range(Y) for c in range(2)] for z in range(Z)
]


def moved(block, target):
    return lax.ppermute(block, "d", [(device_at(*spot), device_at(*target(*spot))) for spot in SPOTS])


def along_z(block, step):
    return moved(block, lambda z, x, y, c: (z + step, x, y, c))


def split_along_z(block, step):
    return moved(block, lambda z, x, y, c: (z + step - 2 * step * c, x, y, c))


def across_lines(block, step):
    return moved(
        block, lambda z, x, y, c: (z, x, y + step, c) if c == 0 else (z, x + step, y, c)
    )


def other_core(block):
    return moved(block, lambda z, x, y, c: (z, x, y, 1 - c))


def swapped_to_all(blocks, groups):
    return lax.all_to_all(blocks, "d", 0, 0, tiled=True, axis_index_groups=groups)


def vmem():
    return pl.BlockSpec(memory_space=pltpu.VMEM)


def smem():
    return pl.BlockSpec(memory_space=pltpu.SMEM)


def call(body, n_in, outs, scratch=(), limit=8):
    return pl.pallas_call(
        body,
        in_specs=[smem()] + [vmem()] * n_in,
        out_specs=jax.tree.map(lambda _: vmem(), outs),
        out_shape=outs,
        scratch_shapes=list(scratch),
        compiler_params=pltpu.CompilerParams(vmem_limit_bytes=limit * 1024 * 1024),
    )


def prepare_body(at, emb, labels, keys, anchors):
    values = emb[...].astype(F32)
    scale = lax.rsqrt(jnp.sum(values * values, axis=1, keepdims=True) + 1e-06)
    unit = (values * scale).astype(BF16)
    for k in range(4):
        keys[k, :KEYS, :] = unit
    anchors[:A_DEV, :] = unit[:A_DEV]
    label = jnp.broadcast_to(labels[...], (8, KEYS))
    high = (label + 256) >> 9
    low = label - high * 512
    top = lax.broadcasted_iota(jnp.int32, (8, KEYS), 0) == 0
    lane = lax.broadcasted_iota(jnp.int32, (8, KEYS), 1)
    blank = jnp.zeros((8, D - 2 * KEYS), BF16)
    for k in range(4):
        keys[k, KEYS:, 2 * KEYS :] = blank
    anchors[A_DEV:, 2 * KEYS :] = blank
    for k, digit in enumerate((high, low)):
        digit = jnp.where(top, digit.astype(F32), 0.0)
        for copy in range(4):
            keys[copy, KEYS:, k * KEYS : (k + 1) * KEYS] = digit.astype(BF16)
        mine = pltpu.roll(jnp.where(lane < A_DEV, digit, 0.0), at[0] * A_DEV, 1)
        anchors[A_DEV:, k * KEYS : (k + 1) * KEYS] = mine.astype(BF16)


def far_body(at, own, before, after, across, far):
    zh = at[0]
    tail = None
    for step, ref in ((0, own), (3, before), (1, after), (2, across)):
        slot = (zh + step) % 4
        far[pl.ds(pl.multiple_of(slot * A_DEV, A_DEV), A_DEV), :] = ref[:A_DEV, :]
        label = ref[A_DEV:, :].astype(F32)
        tail = label if tail is None else tail + label
    far[KEYS:, :] = tail.astype(BF16)


def keys_body(at, line, plus, minus, two, keys):
    for k, ref in enumerate((line, plus, minus, two)):
        keys[k] = ref[...]


def anchors_body(at, far, ahead, across, behind, anchors):
    row = lax.broadcasted_iota(jnp.int32, (LAB, D), 0)
    tail = jnp.zeros((LAB, D), F32)
    for d, ref in enumerate((far, ahead, across, behind)):
        anchors[d * KEYS : (d + 1) * KEYS, :] = ref[:KEYS, :]
        label = jnp.broadcast_to(ref[KEYS:, :].astype(F32)[:1], (LAB, D))
        tail = jnp.where(row == d, label, tail)
    anchors[4 * KEYS :, :] = tail.astype(BF16)


def label_of(rows):
    rows = rows.astype(F32)
    return rows[:, :KEYS] * 512.0 + rows[:, KEYS : 2 * KEYS]


def scores_of(at, keys, anchors, totals, has_own):
    n = KEYS
    labels = label_of(anchors[4 * n :, :])
    if has_own:
        row = lax.broadcasted_iota(jnp.int32, (n, n), 0)
        lane = lax.broadcasted_iota(jnp.int32, (n, n), 1)
        diagonal = (row < A_DEV) & (row + at[0] * A_DEV == lane)

    def product(p, half):
        rows = keys[p][2 * half : 2 * half + 2, :n, :].reshape(2 * n, D)
        return lax.dot_general(
            rows, anchors[: 4 * n, :], (((1,), (1,)), ((), ())), preferred_element_type=F32
        )

    order = [(p, half) for p in range(4) for half in range(2)]
    following = product(*order[0])
    for k, (p, half) in enumerate(order):
        raw = following
        if k + 1 < len(order):
            following = product(*order[k + 1])
        for b in range(2):
            key_label = label_of(keys[p][2 * half + b, n:, :])[:1]
            key_label = jnp.broadcast_to(key_label, (n, n)).T
            for d in range(4):
                dots = raw[b * n : (b + 1) * n, d * n : (d + 1) * n]
                expo = jnp.exp(dots * 10.0 - 10.0)
                positive = key_label == labels[d : d + 1]
                if has_own and p == 0 and d == 0:
                    itself = diagonal & (at[2] == 2 * half + b)
                    expo = jnp.where(itself, 0.0, expo)
                    positive = positive & jnp.logical_not(itself)
                parts = (expo, jnp.where(positive, dots, 0.0), jnp.where(positive, 1.0, 0.0))
                for m, part in enumerate(parts):
                    totals[d][m] += part.reshape(n // 8, 8, n).sum(axis=0)


def mine_body(at, keys, anchors, out):
    totals = [[jnp.zeros((8, KEYS), F32) for _ in range(3)] for _ in range(4)]
    scores_of(at, [keys.at[p] for p in range(4)], anchors, totals, True)
    for d in range(4):
        for k in range(3):
            out[d, k] = totals[d][k]


def theirs_body(at, keys, anchors, before, out):
    totals = [[before[d, k] for k in range(3)] for d in range(4)]
    scores_of(at, [keys.at[p] for p in range(4)], anchors, totals, False)
    for d in range(4):
        slot = (at[1] + d) % 4
        for k in range(3):
            row = jnp.sum(totals[d][k], axis=0, keepdims=True)
            if k == 1:
                row = row * 10.0
            for z in range(Z):
                out[z, k, pl.ds(slot, 1), :] = row


def loss_body(at, arrived, own, both):
    zh, zl = at[0], at[1]
    total = arrived[0]
    for z in range(1, Z):
        total = total + arrived[z]
    denom, pos_sum, count = total[0], total[1], total[2]
    valid = count > 0.0
    loss = jnp.where(valid, jnp.log(denom) + 10.0 - pos_sum / jnp.maximum(count, 1.0), 0.0)
    classes = lax.broadcasted_iota(jnp.int32, loss.shape, 0)
    mine = jnp.sum(jnp.where(classes == zl, loss, 0.0), axis=0, keepdims=True)
    mine = jnp.broadcast_to(mine, (8, KEYS))
    own[...] = pltpu.roll(mine, (4 - zh) % 4 * A_DEV, 1)[0, :A_DEV]
    lane = lax.broadcasted_iota(jnp.int32, (1, KEYS), 1)
    loss_sum = jnp.sum(jnp.sum(loss, axis=0, keepdims=True), axis=1, keepdims=True)
    valid_sum = jnp.sum(
        jnp.sum(jnp.where(valid, 1.0, 0.0), axis=0, keepdims=True), axis=1, keepdims=True
    )
    row = jnp.where(lane == 0, loss_sum, jnp.where(lane == 1, valid_sum, 0.0))
    for k in range(2 * X * Y):
        both[k] = row


def loss_of(embeddings, labels):
    device = lax.axis_index("d")
    c = device % 2
    z = device // 32
    x = device // 4 % 4
    y = device // 16 % 2 * 2 + device // 2 % 2
    at = jnp.stack([z // 4, z % 4, jnp.where(c == 0, x, y), c]).astype(jnp.int32)

    own_keys, own_anchors = call(
        prepare_body,
        2,
        (jax.ShapeDtypeStruct((4, ROWS, D), BF16), jax.ShapeDtypeStruct((SIDE, D), BF16)),
    )(at, embeddings, labels.reshape(1, KEYS))

    line = swapped_to_all(own_keys, LINES)
    across = along_z(own_anchors, 8)

    before = along_z(own_anchors, 4)
    after = along_z(own_anchors, -4)

    plane = []
    for step in (1, -1, 2):
        plane.append(across_lines(line, step))

    (far,) = call(far_body, 4, (jax.ShapeDtypeStruct((ROWS, D), BF16),))(
        at, own_anchors, before, after, across
    )
    across_near = split_along_z(far, 2)
    behind = along_z(far, 1)
    ahead = along_z(far, -1)

    (keys,) = call(keys_body, 4, (jax.ShapeDtypeStruct((4, 4, ROWS, D), BF16),))(at, line, *plane)
    other_keys = other_core(keys)

    column = jax.ShapeDtypeStruct((4 * KEYS + LAB, D), BF16)
    (anchors,) = call(anchors_body, 4, (column,))(at, far, ahead, across_near, behind)
    (first,) = call(mine_body, 2, (jax.ShapeDtypeStruct((4, 3, 8, KEYS), F32),), (), 16)(
        at, keys, anchors
    )
    (sums,) = call(
        theirs_body, 3, (jax.ShapeDtypeStruct((Z, 3, 4, KEYS), F32),), (), 16
    )(at, other_keys, anchors, first)
    arrived = swapped_to_all(sums, COLUMNS)
    own_loss, both = call(
        loss_body,
        1,
        (
            jax.ShapeDtypeStruct((A_DEV,), F32),
            jax.ShapeDtypeStruct((2 * X * Y, 1, KEYS), F32),
        ),
    )(at, arrived)
    anchor_loss, both = lax.optimization_barrier((own_loss, both))
    everyone = swapped_to_all(both, PLANES).sum(axis=0)[0]
    mean_loss = everyone[0] / jnp.maximum(everyone[1], 1.0)
    return (anchor_loss, mean_loss)


def solution(mesh):
    flat = Mesh(mesh.devices.reshape(512), ("d",))
    placed = (P("d", None), P("d"))
    return jax.shard_map(
        loss_of, mesh=flat, in_specs=placed, out_specs=(P("d"), P()), check_vma=False
    )
```

```python
import jax
import jax.numpy as jnp
from jax import lax
from jax.experimental import pallas as pl
from jax.experimental.pallas import tpu as pltpu
from jax.sharding import Mesh
from jax.sharding import PartitionSpec as P

D = 1024
A_DEV = 32
KEYS = 128
LAB = 8
X = 4
Y = 4
Z = 16
ROWS = KEYS + LAB
SIDE = A_DEV + LAB
F32 = jnp.float32
BF16 = jnp.bfloat16


def device_at(z, x, y, c):
    return ((((z % Z) * 2 + (y % Y) // 2) * X + x % X) * 2 + y % 2) * 2 + c


SPOTS = [(z, x, y, c) for z in range(Z) for x in range(X) for y in range(Y) for c in range(2)]
LINES = [[device_at(z, k, y, 0) for k in range(X)] for z in range(Z) for y in range(Y)] + [
    [device_at(z, x, k, 1) for k in range(Y)] for z in range(Z) for x in range(X)
]
COLUMNS = [
    [device_at(z, x, y, c) for z in range(Z)] for x in range(X) for y in range(Y) for c in range(2)
]
PLANES = [
    [device_at(z, x, y, c) for x in range(X) for y in range(Y) for c in range(2)] for z in range(Z)
]


def moved(block, target):
    return lax.ppermute(block, "d", [(device_at(*spot), device_at(*target(*spot))) for spot in SPOTS])


def along_z(block, step):
    return moved(block, lambda z, x, y, c: (z + step, x, y, c))


def split_along_z(block, step):
    return moved(block, lambda z, x, y, c: (z + step - 2 * step * c, x, y, c))


def across_lines(block, step):
    return moved(
        block, lambda z, x, y, c: (z, x, y + step, c) if c == 0 else (z, x + step, y, c)
    )


def other_core(block):
    return moved(block, lambda z, x, y, c: (z, x, y, 1 - c))


def swapped_to_all(blocks, groups):
    return lax.all_to_all(blocks, "d", 0, 0, tiled=True, axis_index_groups=groups)


def vmem():
    return pl.BlockSpec(memory_space=pltpu.VMEM)


def smem():
    return pl.BlockSpec(memory_space=pltpu.SMEM)


def call(body, n_in, outs, scratch=(), limit=8):
    return pl.pallas_call(
        body,
        in_specs=[smem()] + [vmem()] * n_in,
        out_specs=jax.tree.map(lambda _: vmem(), outs),
        out_shape=outs,
        scratch_shapes=list(scratch),
        compiler_params=pltpu.CompilerParams(vmem_limit_bytes=limit * 1024 * 1024),
    )


def prepare_body(at, emb, labels, keys, anchors):
    values = emb[...].astype(F32)
    scale = lax.rsqrt(jnp.sum(values * values, axis=1, keepdims=True) + 1e-06)
    unit = (values * scale).astype(BF16)
    for k in range(4):
        keys[k, :KEYS, :] = unit
    anchors[:A_DEV, :] = unit[:A_DEV]
    label = jnp.broadcast_to(labels[...], (8, KEYS))
    high = (label + 256) >> 9
    low = label - high * 512
    top = lax.broadcasted_iota(jnp.int32, (8, KEYS), 0) == 0
    lane = lax.broadcasted_iota(jnp.int32, (8, KEYS), 1)
    blank = jnp.zeros((8, D - 2 * KEYS), BF16)
    for k in range(4):
        keys[k, KEYS:, 2 * KEYS :] = blank
    anchors[A_DEV:, 2 * KEYS :] = blank
    for k, digit in enumerate((high, low)):
        digit = jnp.where(top, digit.astype(F32), 0.0)
        for copy in range(4):
            keys[copy, KEYS:, k * KEYS : (k + 1) * KEYS] = digit.astype(BF16)
        mine = pltpu.roll(jnp.where(lane < A_DEV, digit, 0.0), at[0] * A_DEV, 1)
        anchors[A_DEV:, k * KEYS : (k + 1) * KEYS] = mine.astype(BF16)


def far_body(at, own, before, after, across, far):
    zh = at[0]
    tail = None
    for step, ref in ((0, own), (3, before), (1, after), (2, across)):
        slot = (zh + step) % 4
        far[pl.ds(pl.multiple_of(slot * A_DEV, A_DEV), A_DEV), :] = ref[:A_DEV, :]
        label = ref[A_DEV:, :].astype(F32)
        tail = label if tail is None else tail + label
    far[KEYS:, :] = tail.astype(BF16)


def rest_body(at, plus, minus, two, rest):
    for k, ref in enumerate((plus, minus, two)):
        rest[k] = ref[...]


def anchors_body(at, far, ahead, across, behind, anchors):
    row = lax.broadcasted_iota(jnp.int32, (LAB, D), 0)
    tail = jnp.zeros((LAB, D), F32)
    for d, ref in enumerate((far, ahead, across, behind)):
        anchors[d * KEYS : (d + 1) * KEYS, :] = ref[:KEYS, :]
        label = jnp.broadcast_to(ref[KEYS:, :].astype(F32)[:1], (LAB, D))
        tail = jnp.where(row == d, label, tail)
    anchors[4 * KEYS :, :] = tail.astype(BF16)


def label_of(rows):
    rows = rows.astype(F32)
    return rows[:, :KEYS] * 512.0 + rows[:, KEYS : 2 * KEYS]


def scores_of(at, keys, anchors, totals, has_own):
    n = KEYS
    labels = label_of(anchors[4 * n :, :])
    if has_own:
        row = lax.broadcasted_iota(jnp.int32, (n, n), 0)
        lane = lax.broadcasted_iota(jnp.int32, (n, n), 1)
        diagonal = (row < A_DEV) & (row + at[0] * A_DEV == lane)

    def product(p, half):
        rows = keys[p][2 * half : 2 * half + 2, :n, :].reshape(2 * n, D)
        return lax.dot_general(
            rows, anchors[: 4 * n, :], (((1,), (1,)), ((), ())), preferred_element_type=F32
        )

    order = [(p, half) for p in range(4) for half in range(2)]
    following = product(*order[0])
    for k, (p, half) in enumerate(order):
        raw = following
        if k + 1 < len(order):
            following = product(*order[k + 1])
        for b in range(2):
            key_label = label_of(keys[p][2 * half + b, n:, :])[:1]
            key_label = jnp.broadcast_to(key_label, (n, n)).T
            for d in range(4):
                dots = raw[b * n : (b + 1) * n, d * n : (d + 1) * n]
                expo = jnp.exp(dots * 10.0 - 10.0)
                positive = key_label == labels[d : d + 1]
                if has_own and p == 0 and d == 0:
                    itself = diagonal & (at[2] == 2 * half + b)
                    expo = jnp.where(itself, 0.0, expo)
                    positive = positive & jnp.logical_not(itself)
                parts = (expo, jnp.where(positive, dots, 0.0), jnp.where(positive, 1.0, 0.0))
                for m, part in enumerate(parts):
                    totals[d][m] += part.reshape(n // 8, 8, n).sum(axis=0)


def mine_body(at, line, rest, anchors, out):
    totals = [[jnp.zeros((8, KEYS), F32) for _ in range(3)] for _ in range(4)]
    scores_of(at, (line, rest.at[0], rest.at[1], rest.at[2]), anchors, totals, True)
    for d in range(4):
        for k in range(3):
            out[d, k] = totals[d][k]


def theirs_body(at, line, rest, anchors, before, out):
    totals = [[before[d, k] for k in range(3)] for d in range(4)]
    scores_of(at, (line, rest.at[0], rest.at[1], rest.at[2]), anchors, totals, False)
    for d in range(4):
        slot = (at[1] + d) % 4
        for k in range(3):
            row = jnp.sum(totals[d][k], axis=0, keepdims=True)
            if k == 1:
                row = row * 10.0
            for z in range(Z):
                out[z, k, pl.ds(slot, 1), :] = row


def loss_body(at, arrived, own, both):
    zh, zl = at[0], at[1]
    total = arrived[0]
    for z in range(1, Z):
        total = total + arrived[z]
    denom, pos_sum, count = total[0], total[1], total[2]
    valid = count > 0.0
    loss = jnp.where(valid, jnp.log(denom) + 10.0 - pos_sum / jnp.maximum(count, 1.0), 0.0)
    classes = lax.broadcasted_iota(jnp.int32, loss.shape, 0)
    mine = jnp.sum(jnp.where(classes == zl, loss, 0.0), axis=0, keepdims=True)
    mine = jnp.broadcast_to(mine, (8, KEYS))
    own[...] = pltpu.roll(mine, (4 - zh) % 4 * A_DEV, 1)[0, :A_DEV]
    lane = lax.broadcasted_iota(jnp.int32, (1, KEYS), 1)
    loss_sum = jnp.sum(jnp.sum(loss, axis=0, keepdims=True), axis=1, keepdims=True)
    valid_sum = jnp.sum(
        jnp.sum(jnp.where(valid, 1.0, 0.0), axis=0, keepdims=True), axis=1, keepdims=True
    )
    row = jnp.where(lane == 0, loss_sum, jnp.where(lane == 1, valid_sum, 0.0))
    for k in range(2 * X * Y):
        both[k] = row


def loss_of(embeddings, labels):
    device = lax.axis_index("d")
    c = device % 2
    z = device // 32
    x = device // 4 % 4
    y = device // 16 % 2 * 2 + device // 2 % 2
    at = jnp.stack([z // 4, z % 4, jnp.where(c == 0, x, y), c]).astype(jnp.int32)

    own_keys, own_anchors = call(
        prepare_body,
        2,
        (jax.ShapeDtypeStruct((4, ROWS, D), BF16), jax.ShapeDtypeStruct((SIDE, D), BF16)),
    )(at, embeddings, labels.reshape(1, KEYS))

    line = swapped_to_all(own_keys, LINES)
    across = along_z(own_anchors, 8)

    before = along_z(own_anchors, 4)
    after = along_z(own_anchors, -4)

    plane = []
    for step in (1, -1, 2):
        plane.append(across_lines(line, step))

    (far,) = call(far_body, 4, (jax.ShapeDtypeStruct((ROWS, D), BF16),))(
        at, own_anchors, before, after, across
    )
    across_near = split_along_z(far, 2)
    behind = along_z(far, 1)
    ahead = along_z(far, -1)

    (rest,) = call(rest_body, 3, (jax.ShapeDtypeStruct((3, 4, ROWS, D), BF16),))(at, *plane)
    other_line = other_core(line)
    other_rest = other_core(rest)

    column = jax.ShapeDtypeStruct((4 * KEYS + LAB, D), BF16)
    (anchors,) = call(anchors_body, 4, (column,))(at, far, ahead, across_near, behind)
    (first,) = call(mine_body, 3, (jax.ShapeDtypeStruct((4, 3, 8, KEYS), F32),), (), 16)(
        at, line, rest, anchors
    )
    (sums,) = call(
        theirs_body, 4, (jax.ShapeDtypeStruct((Z, 3, 4, KEYS), F32),), (), 16
    )(at, other_line, other_rest, anchors, first)
    arrived = swapped_to_all(sums, COLUMNS)
    own_loss, both = call(
        loss_body,
        1,
        (
            jax.ShapeDtypeStruct((A_DEV,), F32),
            jax.ShapeDtypeStruct((2 * X * Y, 1, KEYS), F32),
        ),
    )(at, arrived)
    anchor_loss, both = lax.optimization_barrier((own_loss, both))
    everyone = swapped_to_all(both, PLANES).sum(axis=0)[0]
    mean_loss = everyone[0] / jnp.maximum(everyone[1], 1.0)
    return (anchor_loss, mean_loss)


def solution(mesh):
    flat = Mesh(mesh.devices.reshape(512), ("d",))
    placed = (P("d", None), P("d"))
    return jax.shard_map(
        loss_of, mesh=flat, in_specs=placed, out_specs=(P("d"), P()), check_vma=False
    )
```
